256 devices in a mesh: dp: 8 (over z), expert: 16 (over y, x), tensor: 2 (over core).
Axes of the slice: x: 4, y: 4, z: 8, core: 2. Of those that a mesh axis runs over, the one named last changes fastest.
Arguments:
- tokens: bfloat16 [1536, 7168], P(('dp', 'expert')), may hold values from -6 to 6
- expert_ids: int32 [1536, 8], P(('dp', 'expert')), may hold values from 0 to 15, all different within a row; in each aligned block of 12 rows (0 to 11, 12 to 23, ...) at most 8 rows name the same one
- route_weights: float32 [1536, 8], P(('dp', 'expert')), may hold values from 0.1 to 1
- gate_weights: bfloat16 [16, 7168, 2048], P('expert', 'dp', 'tensor'), may hold values from -0.0625 to 0.0625
- up_weights: bfloat16 [16, 7168, 2048], P('expert', 'dp', 'tensor'), may hold values from -0.0625 to 0.0625
- down_weights: bfloat16 [16, 2048, 7168], P('expert', 'tensor', 'dp'), may hold values from -0.125 to 0.125
- shared_gate: bfloat16 [7168, 2048], P('dp', 'tensor'), may hold values from -0.0625 to 0.0625
- shared_up: bfloat16 [7168, 2048], P('dp', 'tensor'), may hold values from -0.0625 to 0.0625
- shared_down: bfloat16 [2048, 7168], P('tensor', 'dp'), may hold values from -0.125 to 0.125
Outputs:
- mixed: bfloat16 [1536, 7168], P(('dp', 'expert'))
The draws below stay inside these ranges and needn't reach their ends.
Inputs may be any that keep to these rules, and one draw needn't show every extreme that they name: `expert_ids`: each token names 8 different experts. In the rows of one device no expert is named by more than 8 tokens, and in some device's rows some expert is named by exactly 8.
All inputs are finite; a program needn't handle non-finite values.
Results may differ from the reference program's by a relative error of at most 0.005.
Values may be sent and summed in bfloat16 or wider, within the bound.
A program may use at most 128 MiB of HBM per device.

```python
import math
import jax
import jax.numpy as jnp
import numpy as np
from jax import lax

D = 7168
FF = 2048
TOP = 8
EXPERTS = 16
TOK_DEV = 12
CAP = 8
TOKENS = 1536


def block_levels(own_key, shape, shards, smallest, high):
    gain, own = 1.0, jax.random.fold_in(own_key, 6)
    for axis_at, shards_of in shards:
        heights = jnp.exp(jax.random.uniform(jax.random.fold_in(own, axis_at), (shards_of,), jnp.float32, smallest / len(shards), high / len(shards)))
        gain = gain * jnp.repeat(heights, shape[axis_at] // shards_of).reshape([-1 if axis == axis_at else 1 for axis in range(len(shape))])
    return gain


def assign_block(stream_key, own, number, rows, amount, top, limit, skew):
    sequence = jax.random.permutation(stream_key, amount)
    packed, common = shares(amount, rows * top, limit, skew, True), shares(amount, rows * top, limit, skew, False)
    places = jnp.arange(amount)

    def named(lengths, offset_by):
        used = int((lengths > 0).sum())
        fixed = max(1, used // 4)
        passed = fixed + (places - fixed + offset_by * (used - fixed)) % max(1, amount - fixed)
        return jnp.zeros((amount,), jnp.int32).at[sequence[jnp.where(places < fixed, places, passed)]].set(jnp.asarray(lengths, jnp.int32))

    lengths = jnp.where(number % 4 == 0, named(packed, number // 4), named(common, number - number // 4 - 1))
    mixed = jax.random.permutation(jax.random.fold_in(own, 3), amount)
    donor, sink = mixed[0:amount // 2 * 2:2], mixed[1:amount // 2 * 2:2]
    margin = jnp.minimum(lengths[donor] - 1, limit - lengths[sink]) // 2
    margin = jnp.where((donor == sequence[0]) | (sink == sequence[0]) | (lengths[sink] == 0), 0, jnp.maximum(margin, 0))
    passed = jax.random.randint(jax.random.fold_in(own, 4), (amount // 2,), 0, 1 << 20) % (margin + 1)
    lengths = lengths.at[donor].add(-passed).at[sink].add(passed)
    labels = jnp.searchsorted(jnp.cumsum(lengths), jnp.arange(rows * top), side="right").astype(jnp.int32)
    table = labels.reshape(top, rows).T
    table = table[jax.random.permutation(jax.random.fold_in(own, 1), rows)]
    offset_by = jax.random.randint(jax.random.fold_in(own, 2), (rows, 1), 0, top)
    return jnp.take_along_axis(table, (jnp.arange(top)[None, :] + offset_by) % top, axis=1)


def shares(number_of, total, limit, lean, full):
    loads = [(1 << 20) // math.isqrt(grade ** lean) + 1 for grade in range(1, number_of + 1)]
    largest = limit if full else min(limit, max(-(-total // number_of), total * loads[0] // sum(loads)))
    least = 1 if total - largest >= number_of - 1 else 0
    counts, spare = [largest] + [least] * (number_of - 1), total - largest - least * (number_of - 1)
    while spare > 0:
        movable = [i for i in range(1, number_of) if counts[i] < largest] or [i for i in range(1, number_of) if counts[i] < limit]
        mass, remaining = sum([loads[i] for i in movable]), spare
        for i in movable:
            addition = min(limit - counts[i], max(1, remaining * loads[i] // mass), spare)
            counts[i] = counts[i] + addition
            spare = spare - addition
    return np.array(counts)


def noise(key, shape, width, limit, cuts=(), kind=jnp.bfloat16):
    gain = block_levels(key, shape, cuts, -0.22, 0.18) if cuts else 1.0
    array = jax.random.normal(key, shape, jnp.float32) * width * gain
    return jnp.minimum(jnp.maximum(array, -limit), limit).astype(kind)


def setup_inputs(seed: int = 0) -> dict:
    key_of = jax.random.split(jax.random.key(seed), 10)
    tokens = noise(key_of[0], (TOKENS, D), 1.0, 6.0, ((0, 128),))
    expert_ids_keys = jax.random.split(jax.random.fold_in(key_of[1], 1), TOKENS // TOK_DEV)
    expert_ids_turns = jax.random.permutation(jax.random.fold_in(key_of[1], 3), TOKENS // TOK_DEV)
    expert_ids = jax.vmap(lambda own, number: assign_block(jax.random.fold_in(key_of[1], 2), own, number, TOK_DEV, EXPERTS, TOP, CAP, 2))(expert_ids_keys, expert_ids_turns).reshape((TOKENS, TOP))
    route_weights = jnp.clip(jnp.exp(math.log(1.0) - 2.3025851 * jax.random.uniform(key_of[2], (TOKENS, TOP), jnp.float32) ** block_levels(key_of[2], (TOKENS, TOP), ((0, 128),), -0.2, 0.2)), 0.1, 1.0)
    gate_weights = noise(key_of[3], (EXPERTS, D, FF), D ** -0.5, 0.0625, ((0, 16), (1, 8), (2, 2)))
    up_weights = noise(key_of[4], (EXPERTS, D, FF), D ** -0.5, 0.0625, ((0, 16), (1, 8), (2, 2)))
    down_weights = noise(key_of[5], (EXPERTS, FF, D), FF ** -0.5, 0.125, ((0, 16), (1, 2), (2, 8)))
    shared_gate = noise(key_of[6], (D, FF), D ** -0.5, 0.0625, ((0, 8), (1, 2)))
    shared_up = noise(key_of[7], (D, FF), D ** -0.5, 0.0625, ((0, 8), (1, 2)))
    shared_down = noise(key_of[8], (FF, D), FF ** -0.5, 0.125, ((0, 2), (1, 8)))
    return dict(tokens=tokens, expert_ids=expert_ids, route_weights=route_weights, gate_weights=gate_weights, up_weights=up_weights, down_weights=down_weights, shared_gate=shared_gate, shared_up=shared_up, shared_down=shared_down)


def reference(tokens, expert_ids, route_weights, gate_weights, up_weights, down_weights, shared_gate, shared_up, shared_down):
    shared_gate_out = jnp.dot(tokens, shared_gate, preferred_element_type=jnp.float32)
    shared_up_out = jnp.dot(tokens, shared_up, preferred_element_type=jnp.float32)
    shared_hidden = (jax.nn.silu(shared_gate_out) * shared_up_out).astype(jnp.bfloat16)
    shared_out = jnp.dot(shared_hidden, shared_down, preferred_element_type=jnp.float32)

    def accumulate(running, layer_pack):
        gate_matrix, up_matrix, down_matrix, expert_index = layer_pack
        gate_out = jnp.dot(tokens, gate_matrix, preferred_element_type=jnp.float32)
        up_out = jnp.dot(tokens, up_matrix, preferred_element_type=jnp.float32)
        hidden = (jax.nn.silu(gate_out) * up_out).astype(jnp.bfloat16)
        expert_out = jnp.dot(hidden, down_matrix, preferred_element_type=jnp.float32)
        coefficient = jnp.sum(jnp.where(expert_ids == expert_index, route_weights, jnp.zeros_like(route_weights)), axis=1)
        return running + coefficient[:, None] * expert_out.astype(running.dtype), None

    indices = jnp.arange(EXPERTS, dtype=jnp.int32)
    running, unused = lax.scan(accumulate, shared_out, (gate_weights, up_weights, down_weights, indices))
    return running.astype(jnp.bfloat16)
```

```python
import functools

import jax
import jax.numpy as jnp
from jax import lax
from jax.experimental import pallas as pl
from jax.experimental.pallas import tpu as pltpu
from jax.sharding import PartitionSpec as P

CAP = 8
TP = 16
MESH = pl.DeviceIdType.MESH
F32 = jnp.float32
BF16 = jnp.bfloat16


def dot(a, b):
    return jnp.dot(a, b, preferred_element_type=F32)


def layer_kernel(
    Z, E, T, B, FH,
    ids_ref, rw_ref, tok_hbm, wg_hbm, wu_hbm, wd_hbm, sg_hbm, su_hbm, sd_hbm,
    out_ref,
    wg, wu, wd, sg, su, sd,
    tok, tb, tw, xs, xw, pk, x, p, sb, rb, ssb, srb, hid, hs, acc, os_, orc, sac, sos, sor, oo, rr, fb, ob,
    l_sem, t_sem, a_ss, a_rs, w_ss, w_rs, b_ss, b_rs, f_ss, f_rs,
    c_ss, c_rs, d_ss, d_rs, g_ss, g_rs, h_ss, h_rs, o_ss, o_rs, q_ss, q_rs, r_ss, r_rs, y_ss, y_rs,
):
    H = Z // 2
    NS = E * CAP
    z, e, t = lax.axis_index("dp"), lax.axis_index("expert"), lax.axis_index("tensor")
    zr, zl = lax.rem(z + 1, Z), lax.rem(z + Z - 1, Z)
    far = lax.rem(z + H, Z)
    pt = 1 - t

    barrier = pltpu.get_barrier_semaphore()
    for j in range(1, Z):
        zz = lax.rem(z + j, Z)
        for tt in range(2):
            pl.semaphore_signal(barrier, inc=1, device_id=(zz, e, tt), device_id_type=MESH)
    for j in range(1, E):
        ee = lax.rem(e + j, E)
        pl.semaphore_signal(barrier, inc=1, device_id=(z, ee, t), device_id_type=MESH)
    pl.semaphore_signal(barrier, inc=1, device_id=(z, e, pt), device_id_type=MESH)

    def chunk(i, core):
        return lax.rem(z + (1 - core) * (Z - i) + core * (1 + i), Z)

    def at(way, k):
        return lax.rem(z + Z - k, Z) if way == 0 else lax.rem(z + k, Z)

    def owner_home(way, j):
        return lax.rem(z + Z - j + H, Z) if way == 0 else lax.rem(z + j + H, Z)

    def remote(src, dst, ss, rs, dev):
        return pltpu.make_async_remote_copy(
            src_ref=src, dst_ref=dst, send_sem=ss, recv_sem=rs, device_id=dev, device_id_type=MESH
        )

    def next_to(way):
        return (zr if way == 0 else zl, e, t)

    def take(ref, sem):
        pltpu.make_async_copy(ref, ref, sem).wait()

    def rows(j):
        return pl.ds(pl.multiple_of(j * CAP, CAP), CAP)

    tok_load = pltpu.make_async_copy(tok_hbm, tok, t_sem)
    tok_load.start()
    loads = [
        pltpu.make_async_copy(src, dst, l_sem.at[n])
        for n, (src, dst) in enumerate(
            ((sg_hbm, sg), (su_hbm, su), (wg_hbm, wg), (wu_hbm, wu), (wd_hbm, wd), (sd_hbm, sd))
        )
    ]

    ids = ids_ref[...]
    rw = rw_ref[...]
    slot = lax.broadcasted_iota(jnp.int32, (NS, T), 0)
    named = lax.shift_right_logical(slot, 3)
    m = jnp.zeros((NS, T), F32)
    weight = jnp.zeros((NS, T), F32)
    for k in range(ids.shape[0]):
        hit = ids[k : k + 1, :] == named
        m = m + jnp.where(hit, 1.0, 0.0)
        weight = weight + jnp.where(hit, rw[k : k + 1, :], 0.0)
    token = lax.broadcasted_iota(jnp.int32, (NS, T), 1)
    before = jnp.zeros((NS, T), F32)
    for r in range(T - 1):
        before = before + jnp.where(token > r, m[:, r : r + 1], 0.0)
    placed = jnp.where(before == (slot & 7).astype(F32), weight, 0.0)
    tw[...] = jnp.concatenate([placed, jnp.zeros((NS, NS - T), F32)], axis=1).T[0:TP, :]
    for d in range(Z):
        tb[d, 8:TP, :] = jnp.zeros((TP - 8, B), BF16)
    tok_load.wait()
    for load in loads:
        load.start()
    for d in range(Z):
        tb[d, 0:T, :] = tok[:, d * B : (d + 1) * B]

    pl.semaphore_wait(barrier, 2 * (Z - 1) + (E - 1) + 1)

    def target_a(i):
        return lax.rem(z + (1 - t) * i + t * (Z - 1 - i), Z)

    def copy_a(i, tt):
        return remote(tb.at[target_a(i)], xs.at[z], a_ss.at[i, tt], a_rs.at[t, i], (target_a(i), e, tt))

    def copy_w(i):
        return remote(tw, xw.at[i], w_ss.at[i], w_rs.at[i], (target_a(i), e, t))

    def start_a(i):
        copy_a(i, 0).start()
        copy_a(i, 1).start()
        copy_w(i).start()

    def pick(i):
        zc = chunk(i, t)
        cb = jnp.where(xw[i] > 0.0, 1.0, 0.0).astype(BF16)
        picked = lax.dot_general(cb, xs[zc], (((0,), (0,)), ((), ())), preferred_element_type=F32)
        pk[i] = picked.astype(BF16)

        def send_b(k, carry):
            ee = lax.rem(e + k, E)
            remote(pk.at[i, rows(ee)], x.at[zc, rows(e)], b_ss.at[i], b_rs.at[i], (z, ee, t)).start()
            return carry

        lax.fori_loop(1, E, send_b, 0)
        x[zc, rows(e), :] = pk[i, rows(e), :]

    def copy_d(way, k, half):
        return remote(
            ssb.at[way, k, half], srb.at[way, k, half], d_ss.at[way, k, half], d_rs.at[way, k, half], next_to(way)
        )

    def cols(half):
        return slice(half * FH, (half + 1) * FH)

    def step_s(k):
        for half in range(2):
            ways = (half,) if k == 0 else (0, 1)
            v = [xs[at(way, k)] for way in ways]
            v = v[0] if k == 0 else jnp.concatenate(v, axis=0)
            sums = [dot(v, w[:, cols(half)]) for w in (sg, su)]
            for n, way in enumerate(ways):
                if k > 1 or (k == 1 and half == way):
                    copy_d(way, k - 1, half).wait_recv()
                for q in range(2):
                    u = sums[q][n * TP : (n + 1) * TP]
                    if k > 1 or (k == 1 and half == way):
                        u = u + srb[way, k - 1, half, :, cols(q)].astype(F32)
                    ssb[way, k, half, :, cols(q)] = u.astype(BF16)
                copy_d(way, k, half).start()

    def silu_up(g, u):
        return (g / (1.0 + jnp.exp(-g)) * u).astype(BF16)

    def last_s():
        for half in range(2):
            for way in range(2):
                copy_d(way, H - 1, half).wait_recv()
            g, u = [
                dot(xs[far], w[:, cols(half)])
                + srb[0, H - 1, half, :, cols(q)].astype(F32)
                + srb[1, H - 1, half, :, cols(q)].astype(F32)
                for q, w in enumerate((sg, su))
            ]
            hs[far, half] = silu_up(g, u)

    @pl.when(t == 1)
    def _():
        start_a(0)

    for i in range(1, H):
        start_a(i)
    xs[z] = tb[z]

    @pl.when(t == 0)
    def _():
        xw[0] = tw[...]
        pick(0)

    for load in loads[:2]:
        load.wait()
    step_s(0)
    for k in range(1, H):
        take(xs.at[0], a_rs.at[0, k])
        take(xs.at[0], a_rs.at[1, k - 1])
        take(xw.at[0], w_rs.at[k - t])
        pick(k - t)
        if k == 1 and H > 2:
            step_s(1)
    take(xs.at[0], a_rs.at[1, H - 1])

    @pl.when(t == 1)
    def _():
        take(xw.at[0], w_rs.at[H - 1])
        pick(H - 1)

    for k in range(2, H - 1):
        step_s(k)
    for load in loads[2:4]:
        load.wait()

    def copy_c(way, k, half, q):
        return remote(
            sb.at[way, k, half, q],
            rb.at[way, k, half, q],
            c_ss.at[way, k, half, q],
            c_rs.at[way, k, half, q],
            next_to(way),
        )

    def forward(n):
        zc = chunk(n, t)
        return remote(x.at[zc], x.at[zc], f_ss.at[n], f_rs.at[n], (z, e, pt))

    def pass_on(n):
        take(x.at[chunk(n, t), pl.ds(0, (E - 1) * CAP)], b_rs.at[n])
        forward(n).start()

    def from_partner(n):
        take(x.at[chunk(n, pt)], f_rs.at[n])

    def partial(c, half, q, to):
        p[to, q] = dot(x[c], (wg, wu)[q][:, cols(half)])

    @pl.when(t == 0)
    def _():
        pass_on(0)

    @pl.when(t == 1)
    def _():
        from_partner(0)

    for q in range(2):
        for way in range(2):
            partial(z, way, q, way)
            sb[way, 0, way, q] = p[way, q].astype(BF16)
            copy_c(way, 0, way, q).start()
    step_s(H - 1)

    def step_c(k, carry):
        pass_on(k - t)
        from_partner(k - pt)
        for half in range(2):
            for q in range(2):
                for way in range(2):
                    partial(at(way, k), half, q, way)

                    def plus(half=half, q=q, way=way):
                        copy_c(way, k - 1, half, q).wait_recv()
                        p[way, q] = p[way, q] + rb[way, k - 1, half, q].astype(F32)

                    if half == way:
                        plus()
                    else:
                        pl.when(k > 1)(plus)
                    sb[way, k, half, q] = p[way, q].astype(BF16)
                    copy_c(way, k, half, q).start()
        return carry

    lax.fori_loop(1, H, step_c, 0)

    @pl.when(t == 1)
    def _():
        pass_on(H - 1)

    @pl.when(t == 0)
    def _():
        from_partner(H - 1)

    def copy_g(way, half, j):
        c = owner_home(way, j)
        return remote(
            hid.at[c, half], hid.at[c, half], g_ss.at[way, half, j], g_rs.at[way, half, j], next_to(way)
        )

    def copy_h(way, half, j):
        c = owner_home(way, j)
        return remote(hs.at[c, half], hs.at[c, half], h_ss.at[way, half, j], h_rs.at[way, half, j], next_to(way))

    def hop(copy, way, half, j):
        copy(way, half, j - 1).wait_recv()
        if j < H - 1 or (j == H - 1 and half == way):
            copy(way, half, j).start()

    for half in range(2):
        for q in range(2):
            partial(far, half, q, half)
    last_s()
    for half in range(2):
        for q in range(2):
            for way in range(2):
                copy_c(way, H - 1, half, q).wait_recv()
            p[half, q] = p[half, q] + rb[0, H - 1, half, q].astype(F32) + rb[1, H - 1, half, q].astype(F32)
        hid[far, half] = silu_up(p[half, 0], p[half, 1])
        for way in range(2):
            copy_g(way, half, 0).start()

    for load in loads[4:]:
        load.wait()

    def down(v, w):
        return dot(v[0], w[0:FH, :]) + dot(v[1], w[FH : 2 * FH, :])

    def copy_o(i):
        return remote(os_.at[i], orc.at[i], o_ss.at[i], o_rs.at[i], (z, e, pt))

    def copy_q(i):
        return remote(sos.at[i], sor.at[i], q_ss.at[i], q_rs.at[i], (z, e, pt))

    def keep_or_give(i, keeper, c):
        @pl.when(t == keeper)
        def _():
            acc[i] = down(hid[c], wd)

        @pl.when(t != keeper)
        def _():
            os_[i] = down(hid[c], wd)
            copy_o(i).start()

    def shared_one(i, keeper, c):
        v = down(hs[c], sd)

        @pl.when(t == keeper)
        def _():
            sac[i] = v

        @pl.when(t != keeper)
        def _():
            sos[i] = v
            copy_q(i).start()

    def shared_pair(theirs, mine):
        v = jnp.concatenate([hs[chunk(theirs, pt)], hs[chunk(mine, t)]], axis=1)
        v = down(v, sd)
        sos[theirs] = v[0:TP]
        copy_q(theirs).start()
        sac[mine] = v[TP : 2 * TP]

    def finish(i):
        copy_o(i).wait_recv()
        oo[i] = acc[i] + orc[i]

        def send_r(k, carry):
            ee = lax.rem(e + k, E)
            remote(oo.at[i, rows(ee)], rr.at[i, rows(e)], r_ss.at[i], r_rs.at[i], (z, ee, t)).start()
            return carry

        lax.fori_loop(1, E, send_r, 0)
        rr[i, rows(e), :] = oo[i, rows(e), :]

    keep_or_give(H - 1, 1, far)
    for j in range(1, H):
        mine = H - j - t
        theirs = H - j - pt
        for way in range(2):
            hop(copy_g, way, 0, j)
        if j > 1:
            finish(mine + 1)
        for way in range(2):
            hop(copy_g, way, 1, j)
        for half in range(2):
            for way in range(2):
                if j == 1:
                    copy_h(way, half, 0).start()
                else:
                    hop(copy_h, way, half, j - 1)
        os_[theirs] = down(hid[chunk(theirs, pt)], wd)
        copy_o(theirs).start()
        acc[mine] = down(hid[chunk(mine, t)], wd)
        if j == 1:
            shared_one(H - 1, 1, far)

            @pl.when(t == 1)
            def _():
                finish(H - 1)

        else:
            shared_pair(theirs + 1, mine + 1)
    finish(1 - t)
    for half in range(2):
        for way in range(2):
            hop(copy_h, way, half, H - 1)
    copy_g(0, 0, H - 1).wait_recv()
    copy_g(1, 1, H - 1).wait_recv()
    keep_or_give(0, 0, z)
    shared_pair(1 - pt, 1 - t)

    @pl.when(t == 0)
    def _():
        finish(0)

    copy_h(0, 0, H - 1).wait_recv()
    copy_h(1, 1, H - 1).wait_recv()
    shared_one(0, 0, z)

    def copy_y(i, tt):
        return remote(fb.at[i], ob.at[z], y_ss.at[i, tt], y_rs.at[t, i], (chunk(i, t), e, tt))

    def combine(i):
        take(sor.at[i], q_rs.at[i])
        shared = sac[i] + sor[i]
        take(rr.at[i, pl.ds(0, (E - 1) * CAP)], r_rs.at[i])
        v = lax.dot_general(
            xw[i], rr[i], (((1,), (0,)), ((), ())), precision=lax.Precision.HIGHEST, preferred_element_type=F32
        )
        fb[i] = (v + shared).astype(BF16)

    for i in range(H - 1, -1, -1):
        combine(i)
        copy_y(i, 1).start()
        if i > 0:
            copy_y(i, 0).start()
        else:

            @pl.when(t == 1)
            def _():
                copy_y(0, 0).start()

            @pl.when(t == 0)
            def _():
                ob[z] = fb[0]

    for src in range(2):
        for i in range(H):
            if src == 0 and i == 0:

                @pl.when(t == 1)
                def _():
                    take(ob.at[0], y_rs.at[0, 0])

            else:
                take(ob.at[0], y_rs.at[src, i])
    for d in range(Z):
        out_ref[:, d * B : (d + 1) * B] = ob[d, 0:T, :]

    def sent_a(i):
        copy_a(i, 0).wait_send()
        copy_a(i, 1).wait_send()
        copy_w(i).wait_send()

    for i in range(H):
        take(pk.at[i, pl.ds(0, (E - 1) * CAP)], b_ss.at[i])
        take(oo.at[i, pl.ds(0, (E - 1) * CAP)], r_ss.at[i])
        forward(i).wait_send()
        copy_o(i).wait_send()
        copy_q(i).wait_send()
        copy_y(i, 1).wait_send()
        if i > 0:
            copy_y(i, 0).wait_send()
            sent_a(i)

    @pl.when(t == 1)
    def _():
        copy_y(0, 0).wait_send()
        sent_a(0)

    for k in range(H):
        for half in range(2):
            for way in range(2):
                if k > 0 or half == way:
                    copy_d(way, k, half).wait_send()
                    for q in range(2):
                        copy_c(way, k, half, q).wait_send()
                if k < H - 1 or half == way:
                    copy_g(way, half, k).wait_send()
                    copy_h(way, half, k).wait_send()


def solution(mesh):
    Z, E = mesh.shape["dp"], mesh.shape["expert"]
    H, NS = Z // 2, E * CAP

    def per_device(tokens, ids, rw, wg, wu, wd, sg, su, sd):
        T, D = tokens.shape
        B, F = sg.shape
        FH = F // 2
        dma = pltpu.SemaphoreType.DMA
        vm = pl.BlockSpec(memory_space=pltpu.VMEM)
        hbm = pl.BlockSpec(memory_space=pl.ANY)
        return pl.pallas_call(
            functools.partial(layer_kernel, Z, E, T, B, FH),
            out_shape=jax.ShapeDtypeStruct((T, D), BF16),
            in_specs=[vm] * 2 + [hbm] * 7,
            out_specs=vm,
            scratch_shapes=[
                pltpu.VMEM((B, F), BF16),
                pltpu.VMEM((B, F), BF16),
                pltpu.VMEM((F, B), BF16),
                pltpu.VMEM((B, F), BF16),
                pltpu.VMEM((B, F), BF16),
                pltpu.VMEM((F, B), BF16),
                pltpu.VMEM((T, D), BF16),
                pltpu.VMEM((Z, TP, B), BF16),
                pltpu.VMEM((TP, NS), F32),
                pltpu.VMEM((Z, TP, B), BF16),
                pltpu.VMEM((H, TP, NS), F32),
                pltpu.VMEM((H, NS, B), BF16),
                pltpu.VMEM((Z, NS, B), BF16),
                pltpu.VMEM((2, 2, NS, FH), F32),
                pltpu.VMEM((2, H, 2, 2, NS, FH), BF16),
                pltpu.VMEM((2, H, 2, 2, NS, FH), BF16),
                pltpu.VMEM((2, H, 2, TP, F), BF16),
                pltpu.VMEM((2, H, 2, TP, F), BF16),
                pltpu.VMEM((Z, 2, NS, FH), BF16),
                pltpu.VMEM((Z, 2, TP, FH), BF16),
                pltpu.VMEM((H, NS, B), F32),
                pltpu.VMEM((H, NS, B), F32),
                pltpu.VMEM((H, NS, B), F32),
                pltpu.VMEM((H, TP, B), F32),
                pltpu.VMEM((H, TP, B), F32),
                pltpu.VMEM((H, TP, B), F32),
                pltpu.VMEM((H, NS, B), F32),
                pltpu.VMEM((H, NS, B), F32),
                pltpu.VMEM((H, TP, B), BF16),
                pltpu.VMEM((Z, TP, B), BF16),
                dma((6,)), dma(()),
                dma((H, 2)), dma((2, H)), dma((H,)), dma((H,)), dma((H,)), dma((H,)), dma((H,)), dma((H,)),
                dma((2, H, 2, 2)), dma((2, H, 2, 2)), dma((2, H, 2)), dma((2, H, 2)),
                dma((2, 2, H)), dma((2, 2, H)), dma((2, 2, H)), dma((2, 2, H)),
                dma((H,)), dma((H,)), dma((H,)), dma((H,)), dma((H,)), dma((H,)), dma((H, 2)), dma((2, H)),
            ],
            compiler_params=pltpu.CompilerParams(
                collective_id=0, has_side_effects=True, vmem_limit_bytes=60 * 1024 * 1024
            ),
            name="moe_layer",
        )(ids.T, rw.T, tokens, wg.reshape(wg.shape[1:]), wu.reshape(wu.shape[1:]), wd.reshape(wd.shape[1:]), sg, su, sd)

    placed = (
        P(("dp", "expert"), None),
        P(("dp", "expert"), None),
        P(("dp", "expert"), None),
        P("expert", "dp", "tensor"),
        P("expert", "dp", "tensor"),
        P("expert", "tensor", "dp"),
        P("dp", "tensor"),
        P("dp", "tensor"),
        P("tensor", "dp"),
    )
    return jax.shard_map(
        per_device, mesh=mesh, in_specs=placed, out_specs=P(("dp", "expert"), None), check_vma=False
    )
```

```python
import functools

import jax
import jax.numpy as jnp
from jax import lax
from jax.experimental import pallas as pl
from jax.experimental.pallas import tpu as pltpu
from jax.sharding import PartitionSpec as P

CAP = 8
TP = 16
MESH = pl.DeviceIdType.MESH
F32 = jnp.float32
BF16 = jnp.bfloat16


def dot(a, b):
    return jnp.dot(a, b, preferred_element_type=F32)


def layer_kernel(
    Z, E, T, B, FH,
    ids_ref, rw_ref, tok_hbm, wg_hbm, wu_hbm, wd_hbm, sg_hbm, su_hbm, sd_hbm,
    out_ref,
    wg, wu, wd, sg, su, sd,
    tok, tb, tw, xs, xw, pk, x, p, sb, rb, ssb, srb, hid, hs, acc, os_, orc, sac, sos, sor, oo, rr, fb, ob,
    l_sem, t_sem, a_ss, a_rs, v_ss, v_rs, w_ss, w_rs, b_ss, b_rs, f_ss, f_rs,
    c_ss, c_rs, d_ss, d_rs, g_ss, g_rs, h_ss, h_rs, o_ss, o_rs, q_ss, q_rs, r_ss, r_rs, y_ss, y_rs,
):
    H = Z // 2
    NS = E * CAP
    z, e, t = lax.axis_index("dp"), lax.axis_index("expert"), lax.axis_index("tensor")
    zr, zl = lax.rem(z + 1, Z), lax.rem(z + Z - 1, Z)
    far = lax.rem(z + H, Z)
    pt = 1 - t

    barrier = pltpu.get_barrier_semaphore()
    for j in range(1, Z):
        zz = lax.rem(z + j, Z)
        for tt in range(2):
            pl.semaphore_signal(barrier, inc=1, device_id=(zz, e, tt), device_id_type=MESH)
    for j in range(1, E):
        ee = lax.rem(e + j, E)
        pl.semaphore_signal(barrier, inc=1, device_id=(z, ee, t), device_id_type=MESH)
    pl.semaphore_signal(barrier, inc=1, device_id=(z, e, pt), device_id_type=MESH)

    def chunk(i, core):
        return lax.rem(z + (1 - core) * (Z - i) + core * (1 + i), Z)

    def at(way, k):
        return lax.rem(z + Z - k, Z) if way == 0 else lax.rem(z + k, Z)

    def owner_home(way, j):
        return lax.rem(z + Z - j + H, Z) if way == 0 else lax.rem(z + j + H, Z)

    def remote(src, dst, ss, rs, dev):
        return pltpu.make_async_remote_copy(
            src_ref=src, dst_ref=dst, send_sem=ss, recv_sem=rs, device_id=dev, device_id_type=MESH
        )

    def next_to(way):
        return (zr if way == 0 else zl, e, t)

    def take(ref, sem):
        pltpu.make_async_copy(ref, ref, sem).wait()

    def rows(j):
        return pl.ds(pl.multiple_of(j * CAP, CAP), CAP)

    tok_load = pltpu.make_async_copy(tok_hbm, tok, t_sem)
    tok_load.start()
    loads = [
        pltpu.make_async_copy(src, dst, l_sem.at[n])
        for n, (src, dst) in enumerate(
            ((sg_hbm, sg), (su_hbm, su), (wg_hbm, wg), (wu_hbm, wu), (wd_hbm, wd), (sd_hbm, sd))
        )
    ]

    ids = ids_ref[...]
    rw = rw_ref[...]
    slot = lax.broadcasted_iota(jnp.int32, (NS, T), 0)
    named = lax.shift_right_logical(slot, 3)
    m = jnp.zeros((NS, T), F32)
    weight = jnp.zeros((NS, T), F32)
    for k in range(ids.shape[0]):
        hit = ids[k : k + 1, :] == named
        m = m + jnp.where(hit, 1.0, 0.0)
        weight = weight + jnp.where(hit, rw[k : k + 1, :], 0.0)
    token = lax.broadcasted_iota(jnp.int32, (NS, T), 1)
    before = jnp.zeros((NS, T), F32)
    for r in range(T - 1):
        before = before + jnp.where(token > r, m[:, r : r + 1], 0.0)
    placed = jnp.where(before == (slot & 7).astype(F32), m, 0.0)
    which = jnp.sum(placed * (token + 1).astype(F32), axis=1, keepdims=True) - 1.0
    weight = jnp.sum(placed * weight, axis=1, keepdims=True)
    tw[...] = jnp.concatenate([which, weight, jnp.zeros((NS, NS - 2), F32)], axis=1).T[0:8, :]
    for d in range(Z):
        tb[d, 8:TP, :] = jnp.zeros((TP - 8, B), BF16)
    tok_load.wait()
    for load in loads:
        load.start()
    for d in range(Z):
        tb[d, 0:T, :] = tok[:, d * B : (d + 1) * B]

    pl.semaphore_wait(barrier, 2 * (Z - 1) + (E - 1) + 1)

    def copies_a(i):
        d = lax.rem(z + (1 - t) * i + t * (Z - 1 - i), Z)
        return (
            remote(tw, xw.at[i], w_ss.at[i], w_rs.at[i], (d, e, t)),
            remote(tb.at[d], xs.at[z], a_ss.at[i], a_rs.at[i], (d, e, t)),
        )

    def start_a(i):
        for c in copies_a(i):
            c.start()

    def copy_v(i):
        c = chunk(i, t)
        return remote(xs.at[c], xs.at[c], v_ss.at[i], v_rs.at[i], (z, e, pt))

    def named_by(i):
        return lax.broadcasted_iota(jnp.int32, (TP, NS), 0).astype(F32) == xw[i, 0:1, :]

    def pick(i):
        zc = chunk(i, t)
        cb = jnp.where(named_by(i), 1.0, 0.0).astype(BF16)
        picked = lax.dot_general(cb, xs[zc], (((0,), (0,)), ((), ())), preferred_element_type=F32)
        pk[i] = picked.astype(BF16)

        def send_b(k, carry):
            ee = lax.rem(e + k, E)
            remote(pk.at[i, rows(ee)], x.at[zc, rows(e)], b_ss.at[i], b_rs.at[i], (z, ee, t)).start()
            return carry

        lax.fori_loop(1, E, send_b, 0)
        x[zc, rows(e), :] = pk[i, rows(e), :]

    def arrive(i):
        take(xw.at[i], w_rs.at[i])
        take(xs.at[0], a_rs.at[i])
        copy_v(i).start()
        pick(i)

    def copy_d(way, k, half):
        return remote(
            ssb.at[way, k, half], srb.at[way, k, half], d_ss.at[way, k, half], d_rs.at[way, k, half], next_to(way)
        )

    def cols(half):
        return slice(half * FH, (half + 1) * FH)

    def step_s(k, first):
        if first > 0:
            take(xs.at[0], v_rs.at[k - pt])
        for half in range(2):
            ways = (half,) if first == 0 else (0, 1)
            v = [xs[at(way, k)] for way in ways]
            v = v[0] if first == 0 else jnp.concatenate(v, axis=0)
            sums = [dot(v, w[:, cols(half)]) for w in (sg, su)]
            for n, way in enumerate(ways):
                add = first > 1 or (first == 1 and half == way)
                if add:
                    copy_d(way, k - 1, half).wait_recv()
                for q in range(2):
                    u = sums[q][n * TP : (n + 1) * TP]
                    if add:
                        u = u + srb[way, k - 1, half, :, cols(q)].astype(F32)
                    ssb[way, k, half, :, cols(q)] = u.astype(BF16)
                copy_d(way, k, half).start()

    def silu_up(g, u):
        return (g / (1.0 + jnp.exp(-g)) * u).astype(BF16)

    def last_s():
        @pl.when(t == 0)
        def _():
            take(xs.at[0], v_rs.at[H - 1])

        for half in range(2):
            for way in range(2):
                copy_d(way, H - 1, half).wait_recv()
            g, u = [
                dot(xs[far], w[:, cols(half)])
                + srb[0, H - 1, half, :, cols(q)].astype(F32)
                + srb[1, H - 1, half, :, cols(q)].astype(F32)
                for q, w in enumerate((sg, su))
            ]
            hs[far, half] = silu_up(g, u)

    @pl.when(t == 1)
    def _():
        start_a(0)

    for i in range(1, H):
        start_a(i)
    xs[z] = tb[z]

    @pl.when(t == 0)
    def _():
        xw[0] = tw[...]
        pick(0)

    for load in loads[:2]:
        load.wait()
    step_s(0, 0)
    arrive(1 - t)
    for load in loads[2:4]:
        load.wait()

    def copy_c(way, k, half, q):
        return remote(
            sb.at[way, k, half, q],
            rb.at[way, k, half, q],
            c_ss.at[way, k, half, q],
            c_rs.at[way, k, half, q],
            next_to(way),
        )

    def forward(n):
        zc = chunk(n, t)
        return remote(x.at[zc], x.at[zc], f_ss.at[n], f_rs.at[n], (z, e, pt))

    def pass_on(n):
        take(x.at[chunk(n, t), pl.ds(0, (E - 1) * CAP)], b_rs.at[n])
        forward(n).start()

    def from_partner(n):
        take(x.at[chunk(n, pt)], f_rs.at[n])

    def partial(c, half, q, to):
        p[to, q] = dot(x[c], (wg, wu)[q][:, cols(half)])

    @pl.when(t == 0)
    def _():
        pass_on(0)

    @pl.when(t == 1)
    def _():
        from_partner(0)

    for q in range(2):
        for way in range(2):
            partial(z, way, q, way)
            sb[way, 0, way, q] = p[way, q].astype(BF16)
            copy_c(way, 0, way, q).start()
    for k in range(2, H):
        arrive(k - t)

    @pl.when(t == 1)
    def _():
        arrive(H - 1)

    step_s(1, 1)

    def step_c(k, carry):
        pass_on(k - t)
        from_partner(k - pt)
        for half in range(2):
            for q in range(2):
                for way in range(2):
                    partial(at(way, k), half, q, way)

                    def plus(half=half, q=q, way=way):
                        copy_c(way, k - 1, half, q).wait_recv()
                        p[way, q] = p[way, q] + rb[way, k - 1, half, q].astype(F32)

                    if half == way:
                        plus()
                    else:
                        pl.when(k > 1)(plus)
                    sb[way, k, half, q] = p[way, q].astype(BF16)
                    copy_c(way, k, half, q).start()

        @pl.when(k < H - 1)
        def _():
            step_s(k + 1, 2)

        return carry

    lax.fori_loop(1, H, step_c, 0)

    @pl.when(t == 1)
    def _():
        pass_on(H - 1)

    @pl.when(t == 0)
    def _():
        from_partner(H - 1)

    def copy_g(way, half, j):
        c = owner_home(way, j)
        return remote(
            hid.at[c, half], hid.at[c, half], g_ss.at[way, half, j], g_rs.at[way, half, j], next_to(way)
        )

    def copy_h(way, half, j):
        c = owner_home(way, j)
        return remote(hs.at[c, half], hs.at[c, half], h_ss.at[way, half, j], h_rs.at[way, half, j], next_to(way))

    def hop(copy, way, half, j):
        copy(way, half, j - 1).wait_recv()
        if j < H - 1 or (j == H - 1 and half == way):
            copy(way, half, j).start()

    for half in range(2):
        for q in range(2):
            partial(far, half, q, half)
    last_s()
    for half in range(2):
        for q in range(2):
            for way in range(2):
                copy_c(way, H - 1, half, q).wait_recv()
            p[half, q] = p[half, q] + rb[0, H - 1, half, q].astype(F32) + rb[1, H - 1, half, q].astype(F32)
        hid[far, half] = silu_up(p[half, 0], p[half, 1])
        for way in range(2):
            copy_g(way, half, 0).start()

    for load in loads[4:]:
        load.wait()

    def down(v, w):
        return dot(v[0], w[0:FH, :]) + dot(v[1], w[FH : 2 * FH, :])

    def copy_o(i):
        return remote(os_.at[i], orc.at[i], o_ss.at[i], o_rs.at[i], (z, e, pt))

    def copy_q(i):
        return remote(sos.at[i], sor.at[i], q_ss.at[i], q_rs.at[i], (z, e, pt))

    def keep_or_give(i, keeper, c):
        @pl.when(t == keeper)
        def _():
            acc[i] = down(hid[c], wd)

        @pl.when(t != keeper)
        def _():
            os_[i] = down(hid[c], wd)
            copy_o(i).start()

    def shared_one(i, keeper, c):
        v = down(hs[c], sd)

        @pl.when(t == keeper)
        def _():
            sac[i] = v

        @pl.when(t != keeper)
        def _():
            sos[i] = v
            copy_q(i).start()

    def shared_pair(theirs, mine):
        v = jnp.concatenate([hs[chunk(theirs, pt)], hs[chunk(mine, t)]], axis=1)
        v = down(v, sd)
        sos[theirs] = v[0:TP]
        copy_q(theirs).start()
        sac[mine] = v[TP : 2 * TP]

    def finish(i):
        copy_o(i).wait_recv()
        oo[i] = acc[i] + orc[i]

        def send_r(k, carry):
            ee = lax.rem(e + k, E)
            remote(oo.at[i, rows(ee)], rr.at[i, rows(e)], r_ss.at[i], r_rs.at[i], (z, ee, t)).start()
            return carry

        lax.fori_loop(1, E, send_r, 0)
        rr[i, rows(e), :] = oo[i, rows(e), :]

    keep_or_give(H - 1, 1, far)
    for j in range(1, H):
        mine = H - j - t
        theirs = H - j - pt
        for way in range(2):
            hop(copy_g, way, 0, j)
        if j > 1:
            finish(mine + 1)
        for way in range(2):
            hop(copy_g, way, 1, j)
        for half in range(2):
            for way in range(2):
                if j == 1:
                    copy_h(way, half, 0).start()
                else:
                    hop(copy_h, way, half, j - 1)
        os_[theirs] = down(hid[chunk(theirs, pt)], wd)
        copy_o(theirs).start()
        acc[mine] = down(hid[chunk(mine, t)], wd)
        if j == 1:
            shared_one(H - 1, 1, far)

            @pl.when(t == 1)
            def _():
                finish(H - 1)

        else:
            shared_pair(theirs + 1, mine + 1)
    finish(1 - t)
    for half in range(2):
        for way in range(2):
            hop(copy_h, way, half, H - 1)
    copy_g(0, 0, H - 1).wait_recv()
    copy_g(1, 1, H - 1).wait_recv()
    keep_or_give(0, 0, z)
    shared_pair(1 - pt, 1 - t)

    @pl.when(t == 0)
    def _():
        finish(0)

    copy_h(0, 0, H - 1).wait_recv()
    copy_h(1, 1, H - 1).wait_recv()
    shared_one(0, 0, z)

    def copy_y(i, tt):
        return remote(fb.at[i], ob.at[z], y_ss.at[i, tt], y_rs.at[t, i], (chunk(i, t), e, tt))

    def combine(i):
        take(sor.at[i], q_rs.at[i])
        shared = sac[i] + sor[i]
        take(rr.at[i, pl.ds(0, (E - 1) * CAP)], r_rs.at[i])
        v = lax.dot_general(
            jnp.where(named_by(i), xw[i, 1:2, :], 0.0), rr[i], (((1,), (0,)), ((), ())), precision=lax.Precision.HIGHEST, preferred_element_type=F32
        )
        fb[i] = (v + shared).astype(BF16)

    for i in range(H - 1, -1, -1):
        combine(i)
        copy_y(i, 1).start()
        if i > 0:
            copy_y(i, 0).start()
        else:

            @pl.when(t == 1)
            def _():
                copy_y(0, 0).start()

            @pl.when(t == 0)
            def _():
                ob[z] = fb[0]

    for src in range(2):
        for i in range(H):
            if src == 0 and i == 0:

                @pl.when(t == 1)
                def _():
                    take(ob.at[0], y_rs.at[0, 0])

            else:
                take(ob.at[0], y_rs.at[src, i])
    for d in range(Z):
        out_ref[:, d * B : (d + 1) * B] = ob[d, 0:T, :]

    def sent_a(i):
        for c in copies_a(i):
            c.wait_send()
        copy_v(i).wait_send()

    for i in range(H):
        take(pk.at[i, pl.ds(0, (E - 1) * CAP)], b_ss.at[i])
        take(oo.at[i, pl.ds(0, (E - 1) * CAP)], r_ss.at[i])
        forward(i).wait_send()
        copy_o(i).wait_send()
        copy_q(i).wait_send()
        copy_y(i, 1).wait_send()
        if i > 0:
            copy_y(i, 0).wait_send()
            sent_a(i)

    @pl.when(t == 1)
    def _():
        copy_y(0, 0).wait_send()
        sent_a(0)

    for k in range(H):
        for half in range(2):
            for way in range(2):
                if k > 0 or half == way:
                    copy_d(way, k, half).wait_send()
                    for q in range(2):
                        copy_c(way, k, half, q).wait_send()
                if k < H - 1 or half == way:
                    copy_g(way, half, k).wait_send()
                    copy_h(way, half, k).wait_send()


def solution(mesh):
    Z, E = mesh.shape["dp"], mesh.shape["expert"]
    H, NS = Z // 2, E * CAP

    def per_device(tokens, ids, rw, wg, wu, wd, sg, su, sd):
        T, D = tokens.shape
        B, F = sg.shape
        FH = F // 2
        dma = pltpu.SemaphoreType.DMA
        vm = pl.BlockSpec(memory_space=pltpu.VMEM)
        hbm = pl.BlockSpec(memory_space=pl.ANY)
        return pl.pallas_call(
            functools.partial(layer_kernel, Z, E, T, B, FH),
            out_shape=jax.ShapeDtypeStruct((T, D), BF16),
            in_specs=[vm] * 2 + [hbm] * 7,
            out_specs=vm,
            scratch_shapes=[
                pltpu.VMEM((B, F), BF16),
                pltpu.VMEM((B, F), BF16),
                pltpu.VMEM((F, B), BF16),
                pltpu.VMEM((B, F), BF16),
                pltpu.VMEM((B, F), BF16),
                pltpu.VMEM((F, B), BF16),
                pltpu.VMEM((T, D), BF16),
                pltpu.VMEM((Z, TP, B), BF16),
                pltpu.VMEM((8, NS), F32),
                pltpu.VMEM((Z, TP, B), BF16),
                pltpu.VMEM((H, 8, NS), F32),
                pltpu.VMEM((H, NS, B), BF16),
                pltpu.VMEM((Z, NS, B), BF16),
                pltpu.VMEM((2, 2, NS, FH), F32),
                pltpu.VMEM((2, H, 2, 2, NS, FH), BF16),
                pltpu.VMEM((2, H, 2, 2, NS, FH), BF16),
                pltpu.VMEM((2, H, 2, TP, F), BF16),
                pltpu.VMEM((2, H, 2, TP, F), BF16),
                pltpu.VMEM((Z, 2, NS, FH), BF16),
                pltpu.VMEM((Z, 2, TP, FH), BF16),
                pltpu.VMEM((H, NS, B), F32),
                pltpu.VMEM((H, NS, B), F32),
                pltpu.VMEM((H, NS, B), F32),
                pltpu.VMEM((H, TP, B), F32),
                pltpu.VMEM((H, TP, B), F32),
                pltpu.VMEM((H, TP, B), F32),
                pltpu.VMEM((H, NS, B), F32),
                pltpu.VMEM((H, NS, B), F32),
                pltpu.VMEM((H, TP, B), BF16),
                pltpu.VMEM((Z, TP, B), BF16),
                dma((6,)), dma(()),
                dma((H,)), dma((H,)), dma((H,)), dma((H,)), dma((H,)), dma((H,)), dma((H,)), dma((H,)), dma((H,)), dma((H,)),
                dma((2, H, 2, 2)), dma((2, H, 2, 2)), dma((2, H, 2)), dma((2, H, 2)),
                dma((2, 2, H)), dma((2, 2, H)), dma((2, 2, H)), dma((2, 2, H)),
                dma((H,)), dma((H,)), dma((H,)), dma((H,)), dma((H,)), dma((H,)), dma((H, 2)), dma((2, H)),
            ],
            compiler_params=pltpu.CompilerParams(
                collective_id=0, has_side_effects=True, vmem_limit_bytes=60 * 1024 * 1024
            ),
            name="moe_layer",
        )(ids.T, rw.T, tokens, wg.reshape(wg.shape[1:]), wu.reshape(wu.shape[1:]), wd.reshape(wd.shape[1:]), sg, su, sd)

    placed = (
        P(("dp", "expert"), None),
        P(("dp", "expert"), None),
        P(("dp", "expert"), None),
        P("expert", "dp", "tensor"),
        P("expert", "dp", "tensor"),
        P("expert", "tensor", "dp"),
        P("dp", "tensor"),
        P("dp", "tensor"),
        P("tensor", "dp"),
    )
    return jax.shard_map(
        per_device, mesh=mesh, in_specs=placed, out_specs=P(("dp", "expert"), None), check_vma=False
    )
```

```python
import functools

import jax
import jax.numpy as jnp
from jax import lax
from jax.experimental import pallas as pl
from jax.experimental.pallas import tpu as pltpu
from jax.sharding import PartitionSpec as P

CAP = 8
TP = 16
MESH = pl.DeviceIdType.MESH
F32 = jnp.float32
BF16 = jnp.bfloat16


def dot(a, b):
    return jnp.dot(a, b, preferred_element_type=F32)


CODES = 237.0
LOWEST = 126.0
LOG2E = 1.4426950408889634


def code(v):
    c = jnp.maximum((jnp.log(jnp.abs(v)) * LOG2E + LOWEST) * CODES + 0.5, 0.0).astype(jnp.int32)
    return jnp.where(v < 0.0, -c, c).astype(jnp.int16)


def value(coded):
    c = coded.astype(jnp.int32)
    v = jnp.exp2(jnp.abs(c).astype(F32) * (1.0 / CODES) - LOWEST)
    return jnp.where(c > 0, v, jnp.where(c < 0, -v, 0.0))


def layer_kernel(
    Z, E, T, B, FH,
    ids_ref, rw_ref, tok_hbm, wg_hbm, wu_hbm, wd_hbm, sg_hbm, su_hbm, sd_hbm,
    out_ref,
    wg, wu, wd, sg, su, sd,
    tok, tb, tw, xs, xw, pk, x, p, sb, rb, ssb, srb, hid, hs, acc, os_, orc, sac, sos, sor, oo, rr, fb, ob,
    l_sem, t_sem, a_ss, a_rs, v_ss, v_rs, w_ss, w_rs, b_ss, b_rs, f_ss, f_rs,
    c_ss, c_rs, d_ss, d_rs, g_ss, g_rs, h_ss, h_rs, o_ss, o_rs, q_ss, q_rs, r_ss, r_rs, y_ss, y_rs,
):
    H = Z // 2
    NS = E * CAP
    z, e, t = lax.axis_index("dp"), lax.axis_index("expert"), lax.axis_index("tensor")
    zr, zl = lax.rem(z + 1, Z), lax.rem(z + Z - 1, Z)
    far = lax.rem(z + H, Z)
    pt = 1 - t

    barrier = pltpu.get_barrier_semaphore()
    for j in range(1, Z):
        zz = lax.rem(z + j, Z)
        for tt in range(2):
            pl.semaphore_signal(barrier, inc=1, device_id=(zz, e, tt), device_id_type=MESH)
    for j in range(1, E):
        ee = lax.rem(e + j, E)
        pl.semaphore_signal(barrier, inc=1, device_id=(z, ee, t), device_id_type=MESH)
    pl.semaphore_signal(barrier, inc=1, device_id=(z, e, pt), device_id_type=MESH)

    def chunk(i, core):
        return lax.rem(z + (1 - core) * (Z - i) + core * (1 + i), Z)

    def at(way, k):
        return lax.rem(z + Z - k, Z) if way == 0 else lax.rem(z + k, Z)

    def owner_home(way, j):
        return lax.rem(z + Z - j + H, Z) if way == 0 else lax.rem(z + j + H, Z)

    def remote(src, dst, ss, rs, dev):
        return pltpu.make_async_remote_copy(
            src_ref=src, dst_ref=dst, send_sem=ss, recv_sem=rs, device_id=dev, device_id_type=MESH
        )

    def next_to(way):
        return (zr if way == 0 else zl, e, t)

    def take(ref, sem):
        pltpu.make_async_copy(ref, ref, sem).wait()

    def rows(j):
        return pl.ds(pl.multiple_of(j * CAP, CAP), CAP)

    tok_load = pltpu.make_async_copy(tok_hbm, tok, t_sem)
    tok_load.start()
    loads = [
        pltpu.make_async_copy(src, dst, l_sem.at[n])
        for n, (src, dst) in enumerate(
            ((sg_hbm, sg), (su_hbm, su), (wg_hbm, wg), (wu_hbm, wu), (wd_hbm, wd), (sd_hbm, sd))
        )
    ]

    ids = ids_ref[...]
    rw = rw_ref[...]
    slot = lax.broadcasted_iota(jnp.int32, (NS, T), 0)
    named = lax.shift_right_logical(slot, 3)
    m = jnp.zeros((NS, T), F32)
    weight = jnp.zeros((NS, T), F32)
    for k in range(ids.shape[0]):
        hit = ids[k : k + 1, :] == named
        m = m + jnp.where(hit, 1.0, 0.0)
        weight = weight + jnp.where(hit, rw[k : k + 1, :], 0.0)
    token = lax.broadcasted_iota(jnp.int32, (NS, T), 1)
    before = jnp.zeros((NS, T), F32)
    for r in range(T - 1):
        before = before + jnp.where(token > r, m[:, r : r + 1], 0.0)
    placed = jnp.where(before == (slot & 7).astype(F32), m, 0.0)
    which = jnp.sum(placed * (token + 1).astype(F32), axis=1, keepdims=True) - 1.0
    weight = jnp.sum(placed * weight, axis=1, keepdims=True)
    tw[...] = jnp.concatenate([which, weight, jnp.zeros((NS, NS - 2), F32)], axis=1).T[0:8, :]
    for d in range(Z):
        tb[d, 8:TP, :] = jnp.zeros((TP - 8, B), BF16)
    tok_load.wait()
    for load in loads:
        load.start()
    for d in range(Z):
        tb[d, 0:T, :] = tok[:, d * B : (d + 1) * B]

    pl.semaphore_wait(barrier, 2 * (Z - 1) + (E - 1) + 1)

    def copies_a(i):
        d = lax.rem(z + (1 - t) * i + t * (Z - 1 - i), Z)
        return (
            remote(tw, xw.at[i], w_ss.at[i], w_rs.at[i], (d, e, t)),
            remote(tb.at[d], xs.at[z], a_ss.at[i], a_rs.at[i], (d, e, t)),
        )

    def start_a(i):
        for c in copies_a(i):
            c.start()

    def copy_v(i):
        c = chunk(i, t)
        return remote(xs.at[c], xs.at[c], v_ss.at[i], v_rs.at[i], (z, e, pt))

    def named_by(i):
        return lax.broadcasted_iota(jnp.int32, (TP, NS), 0).astype(F32) == xw[i, 0:1, :]

    def pick(i):
        zc = chunk(i, t)
        cb = jnp.where(named_by(i), 1.0, 0.0).astype(BF16)
        picked = lax.dot_general(cb, xs[zc], (((0,), (0,)), ((), ())), preferred_element_type=F32)
        pk[i] = picked.astype(BF16)

        def send_b(k, carry):
            ee = lax.rem(e + k, E)
            remote(pk.at[i, rows(ee)], x.at[zc, rows(e)], b_ss.at[i], b_rs.at[i], (z, ee, t)).start()
            return carry

        lax.fori_loop(1, E, send_b, 0)
        x[zc, rows(e), :] = pk[i, rows(e), :]

    def arrive(i):
        take(xw.at[i], w_rs.at[i])
        take(xs.at[0], a_rs.at[i])
        copy_v(i).start()
        pick(i)

    def copy_d(way, k, half):
        return remote(
            ssb.at[way, k, half], srb.at[way, k, half], d_ss.at[way, k, half], d_rs.at[way, k, half], next_to(way)
        )

    def cols(half):
        return slice(half * FH, (half + 1) * FH)

    def pack(g, u):
        return jnp.concatenate([g[0:8], u[0:8], g[8:T], u[8:T]], axis=0)

    def step_s(k, first):
        if first > 0:
            take(xs.at[0], v_rs.at[k - pt])
        for half in range(2):
            ways = (half,) if first == 0 else (0, 1)
            v = [xs[at(way, k)] for way in ways]
            v = v[0] if first == 0 else jnp.concatenate(v, axis=0)
            sums = [dot(v, w[:, cols(half)]) for w in (sg, su)]
            for n, way in enumerate(ways):
                add = first > 1 or (first == 1 and half == way)
                if add:
                    copy_d(way, k - 1, half).wait_recv()
                packed = pack(*[u[n * TP : (n + 1) * TP] for u in sums])
                if add:
                    packed = packed + value(srb[way, k - 1, half])
                ssb[way, k, half] = code(packed)
                copy_d(way, k, half).start()

    def silu_up(g, u):
        return (g / (1.0 + jnp.exp(-g)) * u).astype(BF16)

    def last_s():
        @pl.when(t == 0)
        def _():
            take(xs.at[0], v_rs.at[H - 1])

        for half in range(2):
            for way in range(2):
                copy_d(way, H - 1, half).wait_recv()
            m = pack(dot(xs[far], sg[:, cols(half)]), dot(xs[far], su[:, cols(half)]))
            m = m + value(srb[0, H - 1, half]) + value(srb[1, H - 1, half])
            rest = jnp.zeros((TP - T, FH), F32)
            g = jnp.concatenate([m[0:8], m[16 : 8 + T], rest], axis=0)
            u = jnp.concatenate([m[8:16], m[8 + T : 2 * T], rest], axis=0)
            hs[far, half] = silu_up(g, u)

    @pl.when(t == 1)
    def _():
        start_a(0)

    for i in range(1, H):
        start_a(i)
    xs[z] = tb[z]

    @pl.when(t == 0)
    def _():
        xw[0] = tw[...]
        pick(0)

    for load in loads[:2]:
        load.wait()
    step_s(0, 0)
    arrive(1 - t)
    for load in loads[2:4]:
        load.wait()

    def copy_c(way, k, half, q):
        return remote(
            sb.at[way, k, half, q],
            rb.at[way, k, half, q],
            c_ss.at[way, k, half, q],
            c_rs.at[way, k, half, q],
            next_to(way),
        )

    def forward(n):
        zc = chunk(n, t)
        return remote(x.at[zc], x.at[zc], f_ss.at[n], f_rs.at[n], (z, e, pt))

    def pass_on(n):
        take(x.at[chunk(n, t), pl.ds(0, (E - 1) * CAP)], b_rs.at[n])
        forward(n).start()

    def from_partner(n):
        take(x.at[chunk(n, pt)], f_rs.at[n])

    def partial(c, half, q, to):
        p[to, q] = dot(x[c], (wg, wu)[q][:, cols(half)])

    @pl.when(t == 0)
    def _():
        pass_on(0)

    @pl.when(t == 1)
    def _():
        from_partner(0)

    for q in range(2):
        for way in range(2):
            partial(z, way, q, way)
            sb[way, 0, way, q] = code(p[way, q])
            copy_c(way, 0, way, q).start()
    for k in range(2, H):
        arrive(k - t)

    @pl.when(t == 1)
    def _():
        arrive(H - 1)

    step_s(1, 1)

    def step_c(k, carry):
        pass_on(k - t)
        from_partner(k - pt)
        for half in range(2):
            for q in range(2):
                for way in range(2):
                    partial(at(way, k), half, q, way)

                    def plus(half=half, q=q, way=way):
                        copy_c(way, k - 1, half, q).wait_recv()
                        p[way, q] = p[way, q] + value(rb[way, k - 1, half, q])

                    if half == way:
                        plus()
                    else:
                        pl.when(k > 1)(plus)
                    sb[way, k, half, q] = code(p[way, q])
                    copy_c(way, k, half, q).start()

        @pl.when(k < H - 1)
        def _():
            step_s(k + 1, 2)

        return carry

    lax.fori_loop(1, H, step_c, 0)

    @pl.when(t == 1)
    def _():
        pass_on(H - 1)

    @pl.when(t == 0)
    def _():
        from_partner(H - 1)

    def copy_g(way, half, j):
        c = owner_home(way, j)
        return remote(
            hid.at[c, half], hid.at[c, half], g_ss.at[way, half, j], g_rs.at[way, half, j], next_to(way)
        )

    def copy_h(way, half, j):
        c = owner_home(way, j)
        return remote(hs.at[c, half], hs.at[c, half], h_ss.at[way, half, j], h_rs.at[way, half, j], next_to(way))

    def hop(copy, way, half, j):
        copy(way, half, j - 1).wait_recv()
        if j < H - 1 or (j == H - 1 and half == way):
            copy(way, half, j).start()

    for half in range(2):
        for q in range(2):
            partial(far, half, q, half)
    last_s()
    for half in range(2):
        for q in range(2):
            for way in range(2):
                copy_c(way, H - 1, half, q).wait_recv()
            p[half, q] = p[half, q] + value(rb[0, H - 1, half, q]) + value(rb[1, H - 1, half, q])
        hid[far, half] = silu_up(p[half, 0], p[half, 1])
        for way in range(2):
            copy_g(way, half, 0).start()

    for load in loads[4:]:
        load.wait()

    def down(v, w):
        return dot(v[0], w[0:FH, :]) + dot(v[1], w[FH : 2 * FH, :])

    def copy_o(i):
        return remote(os_.at[i], orc.at[i], o_ss.at[i], o_rs.at[i], (z, e, pt))

    def copy_q(i):
        return remote(sos.at[i], sor.at[i], q_ss.at[i], q_rs.at[i], (z, e, pt))

    def keep_or_give(i, keeper, c):
        @pl.when(t == keeper)
        def _():
            acc[i] = down(hid[c], wd)

        @pl.when(t != keeper)
        def _():
            os_[i] = down(hid[c], wd).astype(BF16)
            copy_o(i).start()

    def shared_one(i, keeper, c):
        v = down(hs[c], sd)

        @pl.when(t == keeper)
        def _():
            sac[i] = v

        @pl.when(t != keeper)
        def _():
            sos[i] = v
            copy_q(i).start()

    def shared_pair(theirs, mine):
        v = jnp.concatenate([hs[chunk(theirs, pt)], hs[chunk(mine, t)]], axis=1)
        v = down(v, sd)
        sos[theirs] = v[0:TP]
        copy_q(theirs).start()
        sac[mine] = v[TP : 2 * TP]

    def finish(i):
        copy_o(i).wait_recv()
        oo[i] = (acc[i] + orc[i].astype(F32)).astype(BF16)

        def send_r(k, carry):
            ee = lax.rem(e + k, E)
            remote(oo.at[i, rows(ee)], rr.at[i, rows(e)], r_ss.at[i], r_rs.at[i], (z, ee, t)).start()
            return carry

        lax.fori_loop(1, E, send_r, 0)
        rr[i, rows(e), :] = oo[i, rows(e), :]

    keep_or_give(H - 1, 1, far)
    for j in range(1, H):
        mine = H - j - t
        theirs = H - j - pt
        for way in range(2):
            hop(copy_g, way, 0, j)
        if j > 1:
            finish(mine + 1)
        for way in range(2):
            hop(copy_g, way, 1, j)
        os_[theirs] = down(hid[chunk(theirs, pt)], wd).astype(BF16)
        copy_o(theirs).start()
        acc[mine] = down(hid[chunk(mine, t)], wd)
        for half in range(2):
            for way in range(2):
                if j == 1:
                    copy_h(way, half, 0).start()
                else:
                    hop(copy_h, way, half, j - 1)
        if j == 1:
            shared_one(H - 1, 1, far)

            @pl.when(t == 1)
            def _():
                finish(H - 1)

        else:
            shared_pair(theirs + 1, mine + 1)
    finish(1 - t)
    for half in range(2):
        for way in range(2):
            hop(copy_h, way, half, H - 1)
    copy_g(0, 0, H - 1).wait_recv()
    copy_g(1, 1, H - 1).wait_recv()
    keep_or_give(0, 0, z)
    shared_pair(1 - pt, 1 - t)

    @pl.when(t == 0)
    def _():
        finish(0)

    copy_h(0, 0, H - 1).wait_recv()
    copy_h(1, 1, H - 1).wait_recv()
    shared_one(0, 0, z)

    def copy_y(i, tt):
        return remote(fb.at[i], ob.at[z], y_ss.at[i, tt], y_rs.at[t, i], (chunk(i, t), e, tt))

    def combine(i):
        take(sor.at[i], q_rs.at[i])
        shared = sac[i] + sor[i]
        take(rr.at[i, pl.ds(0, (E - 1) * CAP)], r_rs.at[i])
        v = lax.dot_general(
            jnp.where(named_by(i), xw[i, 1:2, :], 0.0),
            rr[i].astype(F32),
            (((1,), (0,)), ((), ())),
            precision=lax.Precision.HIGHEST,
            preferred_element_type=F32,
        )
        fb[i] = (v + shared).astype(BF16)

    for i in range(H - 1, -1, -1):
        combine(i)
        copy_y(i, 1).start()
        if i > 0:
            copy_y(i, 0).start()
        else:

            @pl.when(t == 1)
            def _():
                copy_y(0, 0).start()

            @pl.when(t == 0)
            def _():
                ob[z] = fb[0]

    for src in range(2):
        for i in range(H):
            if src == 0 and i == 0:

                @pl.when(t == 1)
                def _():
                    take(ob.at[0], y_rs.at[0, 0])

            else:
                take(ob.at[0], y_rs.at[src, i])
    for d in range(Z):
        out_ref[:, d * B : (d + 1) * B] = ob[d, 0:T, :]

    def sent_a(i):
        for c in copies_a(i):
            c.wait_send()
        copy_v(i).wait_send()

    for i in range(H):
        take(pk.at[i, pl.ds(0, (E - 1) * CAP)], b_ss.at[i])
        take(oo.at[i, pl.ds(0, (E - 1) * CAP)], r_ss.at[i])
        forward(i).wait_send()
        copy_o(i).wait_send()
        copy_q(i).wait_send()
        copy_y(i, 1).wait_send()
        if i > 0:
            copy_y(i, 0).wait_send()
            sent_a(i)

    @pl.when(t == 1)
    def _():
        copy_y(0, 0).wait_send()
        sent_a(0)

    for k in range(H):
        for half in range(2):
            for way in range(2):
                if k > 0 or half == way:
                    copy_d(way, k, half).wait_send()
                    for q in range(2):
                        copy_c(way, k, half, q).wait_send()
                if k < H - 1 or half == way:
                    copy_g(way, half, k).wait_send()
                    copy_h(way, half, k).wait_send()


def solution(mesh):
    Z, E = mesh.shape["dp"], mesh.shape["expert"]
    H, NS = Z // 2, E * CAP

    def per_device(tokens, ids, rw, wg, wu, wd, sg, su, sd):
        T, D = tokens.shape
        B, F = sg.shape
        FH = F // 2
        dma = pltpu.SemaphoreType.DMA
        vm = pl.BlockSpec(memory_space=pltpu.VMEM)
        hbm = pl.BlockSpec(memory_space=pl.ANY)
        return pl.pallas_call(
            functools.partial(layer_kernel, Z, E, T, B, FH),
            out_shape=jax.ShapeDtypeStruct((T, D), BF16),
            in_specs=[vm] * 2 + [hbm] * 7,
            out_specs=vm,
            scratch_shapes=[
                pltpu.VMEM((B, F), BF16),
                pltpu.VMEM((B, F), BF16),
                pltpu.VMEM((F, B), BF16),
                pltpu.VMEM((B, F), BF16),
                pltpu.VMEM((B, F), BF16),
                pltpu.VMEM((F, B), BF16),
                pltpu.VMEM((T, D), BF16),
                pltpu.VMEM((Z, TP, B), BF16),
                pltpu.VMEM((8, NS), F32),
                pltpu.VMEM((Z, TP, B), BF16),
                pltpu.VMEM((H, 8, NS), F32),
                pltpu.VMEM((H, NS, B), BF16),
                pltpu.VMEM((Z, NS, B), BF16),
                pltpu.VMEM((2, 2, NS, FH), F32),
                pltpu.VMEM((2, H, 2, 2, NS, FH), jnp.int16),
                pltpu.VMEM((2, H, 2, 2, NS, FH), jnp.int16),
                pltpu.VMEM((2, H, 2, 2 * T, FH), jnp.int16),
                pltpu.VMEM((2, H, 2, 2 * T, FH), jnp.int16),
                pltpu.VMEM((Z, 2, NS, FH), BF16),
                pltpu.VMEM((Z, 2, TP, FH), BF16),
                pltpu.VMEM((H, NS, B), F32),
                pltpu.VMEM((H, NS, B), BF16),
                pltpu.VMEM((H, NS, B), BF16),
                pltpu.VMEM((H, TP, B), F32),
                pltpu.VMEM((H, TP, B), F32),
                pltpu.VMEM((H, TP, B), F32),
                pltpu.VMEM((H, NS, B), BF16),
                pltpu.VMEM((H, NS, B), BF16),
                pltpu.VMEM((H, TP, B), BF16),
                pltpu.VMEM((Z, TP, B), BF16),
                dma((6,)), dma(()),
                dma((H,)), dma((H,)), dma((H,)), dma((H,)), dma((H,)), dma((H,)), dma((H,)), dma((H,)), dma((H,)), dma((H,)),
                dma((2, H, 2, 2)), dma((2, H, 2, 2)), dma((2, H, 2)), dma((2, H, 2)),
                dma((2, 2, H)), dma((2, 2, H)), dma((2, 2, H)), dma((2, 2, H)),
                dma((H,)), dma((H,)), dma((H,)), dma((H,)), dma((H,)), dma((H,)), dma((H, 2)), dma((2, H)),
            ],
            compiler_params=pltpu.CompilerParams(
                collective_id=0, has_side_effects=True, vmem_limit_bytes=60 * 1024 * 1024
            ),
            name="moe_layer",
        )(ids.T, rw.T, tokens, wg.reshape(wg.shape[1:]), wu.reshape(wu.shape[1:]), wd.reshape(wd.shape[1:]), sg, su, sd)

    placed = (
        P(("dp", "expert"), None),
        P(("dp", "expert"), None),
        P(("dp", "expert"), None),
        P("expert", "dp", "tensor"),
        P("expert", "dp", "tensor"),
        P("expert", "tensor", "dp"),
        P("dp", "tensor"),
        P("dp", "tensor"),
        P("tensor", "dp"),
    )
    return jax.shard_map(
        per_device, mesh=mesh, in_specs=placed, out_specs=P(("dp", "expert"), None), check_vma=False
    )
```

```python
import functools

import jax
import jax.numpy as jnp
from jax import lax
from jax.experimental import pallas as pl
from jax.experimental.pallas import tpu as pltpu
from jax.sharding import PartitionSpec as P

CAP = 8
TP = 16
MESH = pl.DeviceIdType.MESH
F32 = jnp.float32
BF16 = jnp.bfloat16


def dot(a, b):
    return jnp.dot(a, b, preferred_element_type=F32)


CODES = 237.0
LOWEST = 126.0
LOG2E = 1.4426950408889634


def code(v):
    c = jnp.maximum((jnp.log(jnp.abs(v)) * LOG2E + LOWEST) * CODES + 0.5, 0.0).astype(jnp.int32)
    return jnp.where(v < 0.0, -c, c).astype(jnp.int16)


def value(coded):
    c = coded.astype(jnp.int32)
    v = jnp.exp2(jnp.abs(c).astype(F32) * (1.0 / CODES) - LOWEST)
    return jnp.where(c > 0, v, jnp.where(c < 0, -v, 0.0))


def layer_kernel(
    Z, E, T, B, FH,
    ids_ref, rw_ref, tok_hbm, wg_hbm, wu_hbm, wd_hbm, sg_hbm, su_hbm, sd_hbm,
    out_ref,
    wg, wu, wd, sg, su, sd,
    tok, tb, tw, xs, xw, pk, x, p, sb, rb, ssb, srb, hid, hs, acc, os_, orc, sac, sos, sor, oo, rr, fb, ob,
    l_sem, t_sem, a_ss, a_rs, v_ss, v_rs, w_ss, w_rs, b_ss, b_rs, f_ss, f_rs,
    c_ss, c_rs, d_ss, d_rs, g_ss, g_rs, h_ss, h_rs, o_ss, o_rs, q_ss, q_rs, r_ss, r_rs, y_ss, y_rs,
):
    H = Z // 2
    NS = E * CAP
    z, e, t = lax.axis_index("dp"), lax.axis_index("expert"), lax.axis_index("tensor")
    zr, zl = lax.rem(z + 1, Z), lax.rem(z + Z - 1, Z)
    far = lax.rem(z + H, Z)
    pt = 1 - t

    barrier = pltpu.get_barrier_semaphore()
    for j in range(1, Z):
        zz = lax.rem(z + j, Z)
        for tt in range(2):
            pl.semaphore_signal(barrier, inc=1, device_id=(zz, e, tt), device_id_type=MESH)
    for j in range(1, E):
        ee = lax.rem(e + j, E)
        pl.semaphore_signal(barrier, inc=1, device_id=(z, ee, t), device_id_type=MESH)
    pl.semaphore_signal(barrier, inc=1, device_id=(z, e, pt), device_id_type=MESH)

    def chunk(i, core):
        return lax.rem(z + (1 - core) * (Z - i) + core * (1 + i), Z)

    def at(way, k):
        return lax.rem(z + Z - k, Z) if way == 0 else lax.rem(z + k, Z)

    def owner_home(way, j):
        return lax.rem(z + Z - j + H, Z) if way == 0 else lax.rem(z + j + H, Z)

    def remote(src, dst, ss, rs, dev):
        return pltpu.make_async_remote_copy(
            src_ref=src, dst_ref=dst, send_sem=ss, recv_sem=rs, device_id=dev, device_id_type=MESH
        )

    def next_to(way):
        return (zr if way == 0 else zl, e, t)

    def take(ref, sem):
        pltpu.make_async_copy(ref, ref, sem).wait()

    def rows(j):
        return pl.ds(pl.multiple_of(j * CAP, CAP), CAP)

    tok_load = pltpu.make_async_copy(tok_hbm, tok, t_sem)
    tok_load.start()
    loads = [
        pltpu.make_async_copy(src, dst, l_sem.at[n])
        for n, (src, dst) in enumerate(
            ((sg_hbm, sg), (su_hbm, su), (wg_hbm, wg), (wu_hbm, wu), (wd_hbm, wd), (sd_hbm, sd))
        )
    ]

    ids = ids_ref[...]
    rw = rw_ref[...]
    slot = lax.broadcasted_iota(jnp.int32, (NS, T), 0)
    named = lax.shift_right_logical(slot, 3)
    m = jnp.zeros((NS, T), F32)
    weight = jnp.zeros((NS, T), F32)
    for k in range(ids.shape[0]):
        hit = ids[k : k + 1, :] == named
        m = m + jnp.where(hit, 1.0, 0.0)
        weight = weight + jnp.where(hit, rw[k : k + 1, :], 0.0)
    token = lax.broadcasted_iota(jnp.int32, (NS, T), 1)
    before = jnp.zeros((NS, T), F32)
    for r in range(T - 1):
        before = before + jnp.where(token > r, m[:, r : r + 1], 0.0)
    placed = jnp.where(before == (slot & 7).astype(F32), m, 0.0)
    which = jnp.sum(placed * (token + 1).astype(F32), axis=1, keepdims=True) - 1.0
    weight = jnp.sum(placed * weight, axis=1, keepdims=True)
    tw[...] = jnp.concatenate([which, weight, jnp.zeros((NS, NS - 2), F32)], axis=1).T[0:8, :]
    for d in range(Z):
        tb[d, 8:TP, :] = jnp.zeros((TP - 8, B), BF16)
    tok_load.wait()
    for load in loads:
        load.start()
    for d in range(Z):
        tb[d, 0:T, :] = tok[:, d * B : (d + 1) * B]

    pl.semaphore_wait(barrier, 2 * (Z - 1) + (E - 1) + 1)

    def copies_a(i):
        d = lax.rem(z + (1 - t) * i + t * (Z - 1 - i), Z)
        return (
            remote(tw, xw.at[i], w_ss.at[i], w_rs.at[i], (d, e, t)),
            remote(tb.at[d], xs.at[z], a_ss.at[i], a_rs.at[i], (d, e, t)),
        )

    def start_a(i):
        for c in copies_a(i):
            c.start()

    def copy_v(i):
        c = chunk(i, t)
        return remote(xs.at[c], xs.at[c], v_ss.at[i], v_rs.at[i], (z, e, pt))

    def named_by(i):
        return lax.broadcasted_iota(jnp.int32, (TP, NS), 0).astype(F32) == xw[i, 0:1, :]

    def pick(i):
        zc = chunk(i, t)
        cb = jnp.where(named_by(i), 1.0, 0.0).astype(BF16)
        picked = lax.dot_general(cb, xs[zc], (((0,), (0,)), ((), ())), preferred_element_type=F32)
        pk[i] = picked.astype(BF16)

        def send_b(k, carry):
            ee = lax.rem(e + k, E)
            remote(pk.at[i, rows(ee)], x.at[zc, rows(e)], b_ss.at[i], b_rs.at[i], (z, ee, t)).start()
            return carry

        lax.fori_loop(1, E, send_b, 0)
        x[zc, rows(e), :] = pk[i, rows(e), :]

    def arrive(i):
        take(xw.at[i], w_rs.at[i])
        take(xs.at[0], a_rs.at[i])
        copy_v(i).start()
        pick(i)

    def copy_d(way, k, half):
        return remote(
            ssb.at[way, k, half], srb.at[way, k, half], d_ss.at[way, k, half], d_rs.at[way, k, half], next_to(way)
        )

    def cols(half):
        return slice(half * FH, (half + 1) * FH)

    def pack(g, u):
        return jnp.concatenate([g[0:8], u[0:8], g[8:T], u[8:T]], axis=0)

    def step_s(k, first):
        if first > 0:
            take(xs.at[0], v_rs.at[k - pt])
        for half in range(2):
            ways = (half,) if first == 0 else (0, 1)
            v = [xs[at(way, k)] for way in ways]
            v = v[0] if first == 0 else jnp.concatenate(v, axis=0)
            sums = [dot(v, w[:, cols(half)]) for w in (sg, su)]
            for n, way in enumerate(ways):
                add = first > 1 or (first == 1 and half == way)
                if add:
                    copy_d(way, k - 1, half).wait_recv()
                packed = pack(*[u[n * TP : (n + 1) * TP] for u in sums])
                if add:
                    packed = packed + value(srb[way, k - 1, half])
                ssb[way, k, half] = code(packed)
                copy_d(way, k, half).start()

    def silu_up(g, u):
        return (g / (1.0 + jnp.exp(-g)) * u).astype(BF16)

    def last_s():
        @pl.when(t == 0)
        def _():
            take(xs.at[0], v_rs.at[H - 1])

        for half in range(2):
            for way in range(2):
                copy_d(way, H - 1, half).wait_recv()
            m = pack(dot(xs[far], sg[:, cols(half)]), dot(xs[far], su[:, cols(half)]))
            m = m + value(srb[0, H - 1, half]) + value(srb[1, H - 1, half])
            rest = jnp.zeros((TP - T, FH), F32)
            g = jnp.concatenate([m[0:8], m[16 : 8 + T], rest], axis=0)
            u = jnp.concatenate([m[8:16], m[8 + T : 2 * T], rest], axis=0)
            hs[far, half] = silu_up(g, u)

    @pl.when(t == 1)
    def _():
        start_a(0)

    for i in range(1, H):
        start_a(i)
    xs[z] = tb[z]

    @pl.when(t == 0)
    def _():
        xw[0] = tw[...]
        pick(0)

    for load in loads[:2]:
        load.wait()
    step_s(0, 0)
    arrive(1 - t)
    for load in loads[2:4]:
        load.wait()

    def copy_c(way, k, half, q):
        return remote(
            sb.at[way, k, half, q],
            rb.at[way, k, half, q],
            c_ss.at[way, k, half, q],
            c_rs.at[way, k, half, q],
            next_to(way),
        )

    def forward(n):
        zc = chunk(n, t)
        return remote(x.at[zc], x.at[zc], f_ss.at[n], f_rs.at[n], (z, e, pt))

    def pass_on(n):
        take(x.at[chunk(n, t), pl.ds(0, (E - 1) * CAP)], b_rs.at[n])
        forward(n).start()

    def from_partner(n):
        take(x.at[chunk(n, pt)], f_rs.at[n])

    def partial(c, half, q, to):
        p[to, q] = dot(x[c], (wg, wu)[q][:, cols(half)])

    @pl.when(t == 0)
    def _():
        pass_on(0)

    @pl.when(t == 1)
    def _():
        from_partner(0)

    for q in range(2):
        for way in range(2):
            partial(z, way, q, way)
            sb[way, 0, way, q] = code(p[way, q])
            copy_c(way, 0, way, q).start()
    for k in range(2, H):
        arrive(k - t)

    @pl.when(t == 1)
    def _():
        arrive(H - 1)

    step_s(1, 1)

    def step_c(k, carry):
        pass_on(k - t)
        from_partner(k - pt)
        for half in range(2):
            for q in range(2):
                for way in range(2):
                    partial(at(way, k), half, q, way)

                    def plus(half=half, q=q, way=way):
                        copy_c(way, k - 1, half, q).wait_recv()
                        p[way, q] = p[way, q] + value(rb[way, k - 1, half, q])

                    if half == way:
                        plus()
                    else:
                        pl.when(k > 1)(plus)
                    sb[way, k, half, q] = code(p[way, q])
                    copy_c(way, k, half, q).start()

        @pl.when(k < H - 1)
        def _():
            step_s(k + 1, 2)

        return carry

    lax.fori_loop(1, H, step_c, 0)

    @pl.when(t == 1)
    def _():
        pass_on(H - 1)

    @pl.when(t == 0)
    def _():
        from_partner(H - 1)

    def copy_g(way, half, j):
        c = owner_home(way, j)
        return remote(
            hid.at[c, half], hid.at[c, half], g_ss.at[way, half, j], g_rs.at[way, half, j], next_to(way)
        )

    def copy_h(way, half, j):
        c = owner_home(way, j)
        return remote(hs.at[c, half], hs.at[c, half], h_ss.at[way, half, j], h_rs.at[way, half, j], next_to(way))

    def hop(copy, way, half, j):
        copy(way, half, j - 1).wait_recv()
        if j < H - 1 or (j == H - 1 and half == way):
            copy(way, half, j).start()

    for half in range(2):
        for q in range(2):
            partial(far, half, q, half)
    last_s()
    for half in range(2):
        for way in range(2):
            copy_h(way, half, 0).start()
    for half in range(2):
        for q in range(2):
            for way in range(2):
                copy_c(way, H - 1, half, q).wait_recv()
            p[half, q] = p[half, q] + value(rb[0, H - 1, half, q]) + value(rb[1, H - 1, half, q])
        hid[far, half] = silu_up(p[half, 0], p[half, 1])
        for way in range(2):
            copy_g(way, half, 0).start()

    for load in loads[4:]:
        load.wait()

    def down(v, w):
        return dot(v[0], w[0:FH, :]) + dot(v[1], w[FH : 2 * FH, :])

    def copy_o(i):
        return remote(os_.at[i], orc.at[i], o_ss.at[i], o_rs.at[i], (z, e, pt))

    def copy_q(i):
        return remote(sos.at[i], sor.at[i], q_ss.at[i], q_rs.at[i], (z, e, pt))

    def keep_or_give(i, keeper, c):
        @pl.when(t == keeper)
        def _():
            acc[i] = down(hid[c], wd)

        @pl.when(t != keeper)
        def _():
            os_[i] = down(hid[c], wd).astype(BF16)
            copy_o(i).start()

    def shared_one(i, keeper, c):
        v = down(hs[c], sd)

        @pl.when(t == keeper)
        def _():
            sac[i] = v

        @pl.when(t != keeper)
        def _():
            sos[i] = v
            copy_q(i).start()

    def shared_pair(theirs, mine):
        v = jnp.concatenate([hs[chunk(theirs, pt)], hs[chunk(mine, t)]], axis=1)
        v = down(v, sd)
        sos[theirs] = v[0:TP]
        copy_q(theirs).start()
        sac[mine] = v[TP : 2 * TP]

    def finish(i):
        copy_o(i).wait_recv()
        oo[i] = (acc[i] + orc[i].astype(F32)).astype(BF16)

        def send_r(k, carry):
            ee = lax.rem(e + k, E)
            remote(oo.at[i, rows(ee)], rr.at[i, rows(e)], r_ss.at[i], r_rs.at[i], (z, ee, t)).start()
            return carry

        lax.fori_loop(1, E, send_r, 0)
        rr[i, rows(e), :] = oo[i, rows(e), :]

    def copy_y(i, tt):
        return remote(fb.at[i], ob.at[z], y_ss.at[i, tt], y_rs.at[t, i], (chunk(i, t), e, tt))

    def combine(i):
        take(sor.at[i], q_rs.at[i])
        shared = sac[i] + sor[i]
        take(rr.at[i, pl.ds(0, (E - 1) * CAP)], r_rs.at[i])
        v = lax.dot_general(
            jnp.where(named_by(i), xw[i, 1:2, :], 0.0),
            rr[i].astype(F32),
            (((1,), (0,)), ((), ())),
            precision=lax.Precision.HIGHEST,
            preferred_element_type=F32,
        )
        fb[i] = (v + shared).astype(BF16)

    def go_home(i):
        combine(i)
        copy_y(i, 1).start()
        if i > 0:
            copy_y(i, 0).start()
        else:

            @pl.when(t == 1)
            def _():
                copy_y(0, 0).start()

            @pl.when(t == 0)
            def _():
                ob[z] = fb[0]

    keep_or_give(H - 1, 1, far)
    shared_one(H - 1, 1, far)
    for j in range(1, H):
        mine = H - j - t
        theirs = H - j - pt
        for way in range(2):
            hop(copy_g, way, 0, j)
        if j > 1:
            finish(mine + 1)
        for way in range(2):
            hop(copy_g, way, 1, j)
        os_[theirs] = down(hid[chunk(theirs, pt)], wd).astype(BF16)
        copy_o(theirs).start()
        acc[mine] = down(hid[chunk(mine, t)], wd)
        for half in range(2):
            for way in range(2):
                hop(copy_h, way, half, j)
        if j == 1:

            @pl.when(t == 1)
            def _():
                finish(H - 1)

        shared_pair(theirs, mine)
    finish(1 - t)
    if H > 2:
        go_home(H - 1)
    copy_g(0, 0, H - 1).wait_recv()
    copy_g(1, 1, H - 1).wait_recv()
    keep_or_give(0, 0, z)
    copy_h(0, 0, H - 1).wait_recv()
    copy_h(1, 1, H - 1).wait_recv()
    shared_one(0, 0, z)

    @pl.when(t == 0)
    def _():
        finish(0)

    for i in range(H - 1 if H == 2 else H - 2, -1, -1):
        go_home(i)

    for src in range(2):
        for i in range(H):
            if src == 0 and i == 0:

                @pl.when(t == 1)
                def _():
                    take(ob.at[0], y_rs.at[0, 0])

            else:
                take(ob.at[0], y_rs.at[src, i])
    for d in range(Z):
        out_ref[:, d * B : (d + 1) * B] = ob[d, 0:T, :]

    def sent_a(i):
        for c in copies_a(i):
            c.wait_send()
        copy_v(i).wait_send()

    for i in range(H):
        take(pk.at[i, pl.ds(0, (E - 1) * CAP)], b_ss.at[i])
        take(oo.at[i, pl.ds(0, (E - 1) * CAP)], r_ss.at[i])
        forward(i).wait_send()
        copy_o(i).wait_send()
        copy_q(i).wait_send()
        copy_y(i, 1).wait_send()
        if i > 0:
            copy_y(i, 0).wait_send()
            sent_a(i)

    @pl.when(t == 1)
    def _():
        copy_y(0, 0).wait_send()
        sent_a(0)

    for k in range(H):
        for half in range(2):
            for way in range(2):
                if k > 0 or half == way:
                    copy_d(way, k, half).wait_send()
                    for q in range(2):
                        copy_c(way, k, half, q).wait_send()
                if k < H - 1 or half == way:
                    copy_g(way, half, k).wait_send()
                    copy_h(way, half, k).wait_send()


def solution(mesh):
    Z, E = mesh.shape["dp"], mesh.shape["expert"]
    H, NS = Z // 2, E * CAP

    def per_device(tokens, ids, rw, wg, wu, wd, sg, su, sd):
        T, D = tokens.shape
        B, F = sg.shape
        FH = F // 2
        dma = pltpu.SemaphoreType.DMA
        vm = pl.BlockSpec(memory_space=pltpu.VMEM)
        hbm = pl.BlockSpec(memory_space=pl.ANY)
        return pl.pallas_call(
            functools.partial(layer_kernel, Z, E, T, B, FH),
            out_shape=jax.ShapeDtypeStruct((T, D), BF16),
            in_specs=[vm] * 2 + [hbm] * 7,
            out_specs=vm,
            scratch_shapes=[
                pltpu.VMEM((B, F), BF16),
                pltpu.VMEM((B, F), BF16),
                pltpu.VMEM((F, B), BF16),
                pltpu.VMEM((B, F), BF16),
                pltpu.VMEM((B, F), BF16),
                pltpu.VMEM((F, B), BF16),
                pltpu.VMEM((T, D), BF16),
                pltpu.VMEM((Z, TP, B), BF16),
                pltpu.VMEM((8, NS), F32),
                pltpu.VMEM((Z, TP, B), BF16),
                pltpu.VMEM((H, 8, NS), F32),
                pltpu.VMEM((H, NS, B), BF16),
                pltpu.VMEM((Z, NS, B), BF16),
                pltpu.VMEM((2, 2, NS, FH), F32),
                pltpu.VMEM((2, H, 2, 2, NS, FH), jnp.int16),
                pltpu.VMEM((2, H, 2, 2, NS, FH), jnp.int16),
                pltpu.VMEM((2, H, 2, 2 * T, FH), jnp.int16),
                pltpu.VMEM((2, H, 2, 2 * T, FH), jnp.int16),
                pltpu.VMEM((Z, 2, NS, FH), BF16),
                pltpu.VMEM((Z, 2, TP, FH), BF16),
                pltpu.VMEM((H, NS, B), F32),
                pltpu.VMEM((H, NS, B), BF16),
                pltpu.VMEM((H, NS, B), BF16),
                pltpu.VMEM((H, TP, B), F32),
                pltpu.VMEM((H, TP, B), F32),
                pltpu.VMEM((H, TP, B), F32),
                pltpu.VMEM((H, NS, B), BF16),
                pltpu.VMEM((H, NS, B), BF16),
                pltpu.VMEM((H, TP, B), BF16),
                pltpu.VMEM((Z, TP, B), BF16),
                dma((6,)), dma(()),
                dma((H,)), dma((H,)), dma((H,)), dma((H,)), dma((H,)), dma((H,)), dma((H,)), dma((H,)), dma((H,)), dma((H,)),
                dma((2, H, 2, 2)), dma((2, H, 2, 2)), dma((2, H, 2)), dma((2, H, 2)),
                dma((2, 2, H)), dma((2, 2, H)), dma((2, 2, H)), dma((2, 2, H)),
                dma((H,)), dma((H,)), dma((H,)), dma((H,)), dma((H,)), dma((H,)), dma((H, 2)), dma((2, H)),
            ],
            compiler_params=pltpu.CompilerParams(
                collective_id=0, has_side_effects=True, vmem_limit_bytes=60 * 1024 * 1024
            ),
            name="moe_layer",
        )(ids.T, rw.T, tokens, wg.reshape(wg.shape[1:]), wu.reshape(wu.shape[1:]), wd.reshape(wd.shape[1:]), sg, su, sd)

    placed = (
        P(("dp", "expert"), None),
        P(("dp", "expert"), None),
        P(("dp", "expert"), None),
        P("expert", "dp", "tensor"),
        P("expert", "dp", "tensor"),
        P("expert", "tensor", "dp"),
        P("dp", "tensor"),
        P("dp", "tensor"),
        P("tensor", "dp"),
    )
    return jax.shard_map(
        per_device, mesh=mesh, in_specs=placed, out_specs=P(("dp", "expert"), None), check_vma=False
    )
```

```python
import functools

import jax
import jax.numpy as jnp
from jax import lax
from jax.experimental import pallas as pl
from jax.experimental.pallas import tpu as pltpu
from jax.sharding import PartitionSpec as P

CAP = 8
TP = 16
MESH = pl.DeviceIdType.MESH
F32 = jnp.float32
BF16 = jnp.bfloat16


def dot(a, b):
    return jnp.dot(a, b, preferred_element_type=F32)


CODES = 237.0
LOWEST = 126.0
LOG2E = 1.4426950408889634


def code(v):
    c = jnp.maximum((jnp.log(jnp.abs(v)) * LOG2E + LOWEST) * CODES + 0.5, 0.0).astype(jnp.int32)
    return jnp.where(v < 0.0, -c, c).astype(jnp.int16)


def value(coded):
    c = coded.astype(jnp.int32)
    v = jnp.exp2(jnp.abs(c).astype(F32) * (1.0 / CODES) - LOWEST)
    return jnp.where(c > 0, v, jnp.where(c < 0, -v, 0.0))


def layer_kernel(
    Z, E, T, B, FH,
    ids_ref, rw_ref, tok_hbm, wg_hbm, wu_hbm, wd_hbm, sg_hbm, su_hbm, sd_hbm,
    out_ref,
    wg, wu, wd, sg, su, sd,
    tok, tb, tw, xs, xw, pk, x, p, sb, rb, ssb, srb, hid, hs, acc, os_, orc, sac, sos, sor, oo, rr, fb, ob,
    l_sem, t_sem, a_ss, a_rs, v_ss, v_rs, w_ss, w_rs, b_ss, b_rs, f_ss, f_rs,
    c_ss, c_rs, d_ss, d_rs, g_ss, g_rs, h_ss, h_rs, o_ss, o_rs, q_ss, q_rs, r_ss, r_rs, y_ss, y_rs,
):
    H = Z // 2
    NS = E * CAP
    z, e, t = lax.axis_index("dp"), lax.axis_index("expert"), lax.axis_index("tensor")
    zr, zl = lax.rem(z + 1, Z), lax.rem(z + Z - 1, Z)
    far = lax.rem(z + H, Z)
    pt = 1 - t

    barrier = pltpu.get_barrier_semaphore()
    for j in range(1, Z):
        zz = lax.rem(z + j, Z)
        for tt in range(2):
            pl.semaphore_signal(barrier, inc=1, device_id=(zz, e, tt), device_id_type=MESH)
    for j in range(1, E):
        ee = lax.rem(e + j, E)
        pl.semaphore_signal(barrier, inc=1, device_id=(z, ee, t), device_id_type=MESH)
    pl.semaphore_signal(barrier, inc=1, device_id=(z, e, pt), device_id_type=MESH)

    def chunk(i, core):
        return lax.rem(z + (1 - core) * (Z - i) + core * (1 + i), Z)

    def at(way, k):
        return lax.rem(z + Z - k, Z) if way == 0 else lax.rem(z + k, Z)

    def owner_home(way, j):
        return lax.rem(z + Z - j + H, Z) if way == 0 else lax.rem(z + j + H, Z)

    def remote(src, dst, ss, rs, dev):
        return pltpu.make_async_remote_copy(
            src_ref=src, dst_ref=dst, send_sem=ss, recv_sem=rs, device_id=dev, device_id_type=MESH
        )

    def next_to(way):
        return (zr if way == 0 else zl, e, t)

    def take(ref, sem):
        pltpu.make_async_copy(ref, ref, sem).wait()

    def rows(j):
        return pl.ds(pl.multiple_of(j * CAP, CAP), CAP)

    tok_load = pltpu.make_async_copy(tok_hbm, tok, t_sem)
    tok_load.start()
    loads = [
        pltpu.make_async_copy(src, dst, l_sem.at[n])
        for n, (src, dst) in enumerate(
            ((sg_hbm, sg), (su_hbm, su), (wg_hbm, wg), (wu_hbm, wu), (wd_hbm, wd), (sd_hbm, sd))
        )
    ]

    ids = ids_ref[...]
    rw = rw_ref[...]
    slot = lax.broadcasted_iota(jnp.int32, (NS, T), 0)
    named = lax.shift_right_logical(slot, 3)
    m = jnp.zeros((NS, T), F32)
    weight = jnp.zeros((NS, T), F32)
    for k in range(ids.shape[0]):
        hit = ids[k : k + 1, :] == named
        m = m + jnp.where(hit, 1.0, 0.0)
        weight = weight + jnp.where(hit, rw[k : k + 1, :], 0.0)
    token = lax.broadcasted_iota(jnp.int32, (NS, T), 1)
    before = jnp.zeros((NS, T), F32)
    for r in range(T - 1):
        before = before + jnp.where(token > r, m[:, r : r + 1], 0.0)
    placed = jnp.where(before == (slot & 7).astype(F32), m, 0.0)
    which = jnp.sum(placed * (token + 1).astype(F32), axis=1, keepdims=True) - 1.0
    weight = jnp.sum(placed * weight, axis=1, keepdims=True)
    tw[...] = jnp.concatenate([which, weight, jnp.zeros((NS, NS - 2), F32)], axis=1).T[0:8, :]
    for d in range(Z):
        tb[d, 8:TP, :] = jnp.zeros((TP - 8, B), BF16)
    tok_load.wait()
    for load in loads:
        load.start()
    for d in range(Z):
        tb[d, 0:T, :] = tok[:, d * B : (d + 1) * B]

    pl.semaphore_wait(barrier, 2 * (Z - 1) + (E - 1) + 1)

    def copies_a(i):
        d = lax.rem(z + (1 - t) * i + t * (Z - 1 - i), Z)
        return (
            remote(tw, xw.at[i], w_ss.at[i], w_rs.at[i], (d, e, t)),
            remote(tb.at[d], xs.at[z], a_ss.at[i], a_rs.at[i], (d, e, t)),
        )

    def start_a(i):
        for c in copies_a(i):
            c.start()

    def copy_v(i):
        c = chunk(i, t)
        return remote(xs.at[c], xs.at[c], v_ss.at[i], v_rs.at[i], (z, e, pt))

    def named_by(i):
        return lax.broadcasted_iota(jnp.int32, (TP, NS), 0).astype(F32) == xw[i, 0:1, :]

    def pick(i):
        zc = chunk(i, t)
        cb = jnp.where(named_by(i), 1.0, 0.0).astype(BF16)
        picked = lax.dot_general(cb, xs[zc], (((0,), (0,)), ((), ())), preferred_element_type=F32)
        pk[i] = picked.astype(BF16)

        def send_b(k, carry):
            ee = lax.rem(e + k, E)
            remote(pk.at[i, rows(ee)], x.at[zc, rows(e)], b_ss.at[i], b_rs.at[i], (z, ee, t)).start()
            return carry

        lax.fori_loop(1, E, send_b, 0)
        x[zc, rows(e), :] = pk[i, rows(e), :]

    def arrive(i):
        take(xw.at[i], w_rs.at[i])
        take(xs.at[0], a_rs.at[i])
        copy_v(i).start()
        pick(i)

    def copy_d(way, k, half):
        return remote(
            ssb.at[way, k, half], srb.at[way, k, half], d_ss.at[way, k, half], d_rs.at[way, k, half], next_to(way)
        )

    def cols(half):
        return slice(half * FH, (half + 1) * FH)

    def pack(g, u):
        return jnp.concatenate([g[0:8], u[0:8], g[8:T], u[8:T]], axis=0)

    def step_s(k, first):
        if first > 0:
            take(xs.at[0], v_rs.at[k - pt])
        for half in range(2):
            ways = (half,) if first == 0 else (0, 1)
            v = [xs[at(way, k)] for way in ways]
            v = v[0] if first == 0 else jnp.concatenate(v, axis=0)
            sums = [dot(v, w[:, cols(half)]) for w in (sg, su)]
            for n, way in enumerate(ways):
                add = first > 1 or (first == 1 and half == way)
                if add:
                    copy_d(way, k - 1, half).wait_recv()
                packed = pack(*[u[n * TP : (n + 1) * TP] for u in sums])
                if add:
                    packed = packed + value(srb[way, k - 1, half])
                ssb[way, k, half] = code(packed)
                copy_d(way, k, half).start()

    def silu_up(g, u):
        return (g / (1.0 + jnp.exp(-g)) * u).astype(BF16)

    def last_s():
        @pl.when(t == 0)
        def _():
            take(xs.at[0], v_rs.at[H - 1])

        for half in range(2):
            for way in range(2):
                copy_d(way, H - 1, half).wait_recv()
            m = pack(dot(xs[far], sg[:, cols(half)]), dot(xs[far], su[:, cols(half)]))
            m = m + value(srb[0, H - 1, half]) + value(srb[1, H - 1, half])
            rest = jnp.zeros((TP - T, FH), F32)
            g = jnp.concatenate([m[0:8], m[16 : 8 + T], rest], axis=0)
            u = jnp.concatenate([m[8:16], m[8 + T : 2 * T], rest], axis=0)
            hs[far, half] = silu_up(g, u)

    xs[z] = tb[z]

    @pl.when(t == 0)
    def _():
        xw[0] = tw[...]
        pick(0)

    @pl.when(t == 1)
    def _():
        start_a(0)

    for i in range(1, H):
        start_a(i)
    for load in loads[:2]:
        load.wait()
    step_s(0, 0)
    arrive(1 - t)
    step_s(1, 1)
    for load in loads[2:4]:
        load.wait()

    def copy_c(way, k, half, q):
        return remote(
            sb.at[way, k, half, q],
            rb.at[way, k, half, q],
            c_ss.at[way, k, half, q],
            c_rs.at[way, k, half, q],
            next_to(way),
        )

    def forward(n):
        zc = chunk(n, t)
        return remote(x.at[zc], x.at[zc], f_ss.at[n], f_rs.at[n], (z, e, pt))

    def pass_on(n):
        take(x.at[chunk(n, t), pl.ds(0, (E - 1) * CAP)], b_rs.at[n])
        forward(n).start()

    def from_partner(n):
        take(x.at[chunk(n, pt)], f_rs.at[n])

    def partial(c, half, q, to):
        p[to, q] = dot(x[c], (wg, wu)[q][:, cols(half)])

    @pl.when(t == 0)
    def _():
        pass_on(0)

    @pl.when(t == 1)
    def _():
        from_partner(0)

    for q in range(2):
        for way in range(2):
            partial(z, way, q, way)
            sb[way, 0, way, q] = code(p[way, q])
            copy_c(way, 0, way, q).start()
    for k in range(2, H):
        arrive(k - t)

    @pl.when(t == 1)
    def _():
        arrive(H - 1)

    def step_c(k, carry):
        pass_on(k - t)
        from_partner(k - pt)
        for half in range(2):
            for q in range(2):
                for way in range(2):
                    partial(at(way, k), half, q, way)

                    def plus(half=half, q=q, way=way):
                        copy_c(way, k - 1, half, q).wait_recv()
                        p[way, q] = p[way, q] + value(rb[way, k - 1, half, q])

                    if half == way:
                        plus()
                    else:
                        pl.when(k > 1)(plus)
                    sb[way, k, half, q] = code(p[way, q])
                    copy_c(way, k, half, q).start()

        @pl.when(k < H - 1)
        def _():
            step_s(k + 1, 2)

        return carry

    lax.fori_loop(1, H, step_c, 0)

    @pl.when(t == 1)
    def _():
        pass_on(H - 1)

    @pl.when(t == 0)
    def _():
        from_partner(H - 1)

    def copy_g(way, half, j):
        c = owner_home(way, j)
        return remote(
            hid.at[c, half], hid.at[c, half], g_ss.at[way, half, j], g_rs.at[way, half, j], next_to(way)
        )

    def copy_h(way, half, j):
        c = owner_home(way, j)
        return remote(hs.at[c, half], hs.at[c, half], h_ss.at[way, half, j], h_rs.at[way, half, j], next_to(way))

    def hop(copy, way, half, j):
        copy(way, half, j - 1).wait_recv()
        if j < H - 1 or (j == H - 1 and half == way):
            copy(way, half, j).start()

    for half in range(2):
        for q in range(2):
            partial(far, half, q, half)
    last_s()
    for half in range(2):
        for way in range(2):
            copy_h(way, half, 0).start()
    for half in range(2):
        for q in range(2):
            for way in range(2):
                copy_c(way, H - 1, half, q).wait_recv()
            p[half, q] = p[half, q] + value(rb[0, H - 1, half, q]) + value(rb[1, H - 1, half, q])
        hid[far, half] = silu_up(p[half, 0], p[half, 1])
        for way in range(2):
            copy_g(way, half, 0).start()

    for load in loads[4:]:
        load.wait()

    def down(v, w):
        return dot(v[0], w[0:FH, :]) + dot(v[1], w[FH : 2 * FH, :])

    def copy_o(i):
        return remote(os_.at[i], orc.at[i], o_ss.at[i], o_rs.at[i], (z, e, pt))

    def copy_q(i):
        return remote(sos.at[i], sor.at[i], q_ss.at[i], q_rs.at[i], (z, e, pt))

    def keep_or_give(i, keeper, c):
        @pl.when(t == keeper)
        def _():
            acc[i] = down(hid[c], wd)

        @pl.when(t != keeper)
        def _():
            os_[i] = down(hid[c], wd).astype(BF16)
            copy_o(i).start()

    def shared_one(i, keeper, c):
        v = down(hs[c], sd)

        @pl.when(t == keeper)
        def _():
            sac[i] = v

        @pl.when(t != keeper)
        def _():
            sos[i] = v
            copy_q(i).start()

    def shared_pair(theirs, mine):
        v = jnp.concatenate([hs[chunk(theirs, pt)], hs[chunk(mine, t)]], axis=1)
        v = down(v, sd)
        sos[theirs] = v[0:TP]
        copy_q(theirs).start()
        sac[mine] = v[TP : 2 * TP]

    def finish(i):
        copy_o(i).wait_recv()
        oo[i] = (acc[i] + orc[i].astype(F32)).astype(BF16)

        def send_r(k, carry):
            ee = lax.rem(e + k, E)
            remote(oo.at[i, rows(ee)], rr.at[i, rows(e)], r_ss.at[i], r_rs.at[i], (z, ee, t)).start()
            return carry

        lax.fori_loop(1, E, send_r, 0)
        rr[i, rows(e), :] = oo[i, rows(e), :]

    def copy_y(i, tt):
        return remote(fb.at[i], ob.at[z], y_ss.at[i, tt], y_rs.at[t, i], (chunk(i, t), e, tt))

    def combine(i):
        take(sor.at[i], q_rs.at[i])
        shared = sac[i] + sor[i]
        take(rr.at[i, pl.ds(0, (E - 1) * CAP)], r_rs.at[i])
        v = lax.dot_general(
            jnp.where(named_by(i), xw[i, 1:2, :], 0.0),
            rr[i].astype(F32),
            (((1,), (0,)), ((), ())),
            precision=lax.Precision.HIGHEST,
            preferred_element_type=F32,
        )
        fb[i] = (v + shared).astype(BF16)

    def go_home(i):
        combine(i)
        copy_y(i, 1).start()
        if i > 0:
            copy_y(i, 0).start()
        else:

            @pl.when(t == 1)
            def _():
                copy_y(0, 0).start()

            @pl.when(t == 0)
            def _():
                ob[z] = fb[0]

    keep_or_give(H - 1, 1, far)
    shared_one(H - 1, 1, far)
    for j in range(1, H):
        mine = H - j - t
        theirs = H - j - pt
        for way in range(2):
            hop(copy_g, way, 0, j)
        if j > 1:
            finish(mine + 1)
        for way in range(2):
            hop(copy_g, way, 1, j)
        os_[theirs] = down(hid[chunk(theirs, pt)], wd).astype(BF16)
        copy_o(theirs).start()
        acc[mine] = down(hid[chunk(mine, t)], wd)
        for half in range(2):
            for way in range(2):
                hop(copy_h, way, half, j)
        if j == 1:

            @pl.when(t == 1)
            def _():
                finish(H - 1)

        shared_pair(theirs, mine)
    finish(1 - t)
    if H > 2:
        go_home(H - 1)
    copy_g(0, 0, H - 1).wait_recv()
    copy_g(1, 1, H - 1).wait_recv()
    keep_or_give(0, 0, z)
    copy_h(0, 0, H - 1).wait_recv()
    copy_h(1, 1, H - 1).wait_recv()
    shared_one(0, 0, z)

    @pl.when(t == 0)
    def _():
        finish(0)

    for i in range(H - 1 if H == 2 else H - 2, -1, -1):
        go_home(i)

    for src in range(2):
        for i in range(H):
            if src == 0 and i == 0:

                @pl.when(t == 1)
                def _():
                    take(ob.at[0], y_rs.at[0, 0])

            else:
                take(ob.at[0], y_rs.at[src, i])
    for d in range(Z):
        out_ref[:, d * B : (d + 1) * B] = ob[d, 0:T, :]

    def sent_a(i):
        for c in copies_a(i):
            c.wait_send()
        copy_v(i).wait_send()

    for i in range(H):
        take(pk.at[i, pl.ds(0, (E - 1) * CAP)], b_ss.at[i])
        take(oo.at[i, pl.ds(0, (E - 1) * CAP)], r_ss.at[i])
        forward(i).wait_send()
        copy_o(i).wait_send()
        copy_q(i).wait_send()
        copy_y(i, 1).wait_send()
        if i > 0:
            copy_y(i, 0).wait_send()
            sent_a(i)

    @pl.when(t == 1)
    def _():
        copy_y(0, 0).wait_send()
        sent_a(0)

    for k in range(H):
        for half in range(2):
            for way in range(2):
                if k > 0 or half == way:
                    copy_d(way, k, half).wait_send()
                    for q in range(2):
                        copy_c(way, k, half, q).wait_send()
                if k < H - 1 or half == way:
                    copy_g(way, half, k).wait_send()
                    copy_h(way, half, k).wait_send()


def solution(mesh):
    Z, E = mesh.shape["dp"], mesh.shape["expert"]
    H, NS = Z // 2, E * CAP

    def per_device(tokens, ids, rw, wg, wu, wd, sg, su, sd):
        T, D = tokens.shape
        B, F = sg.shape
        FH = F // 2
        dma = pltpu.SemaphoreType.DMA
        vm = pl.BlockSpec(memory_space=pltpu.VMEM)
        hbm = pl.BlockSpec(memory_space=pl.ANY)
        return pl.pallas_call(
            functools.partial(layer_kernel, Z, E, T, B, FH),
            out_shape=jax.ShapeDtypeStruct((T, D), BF16),
            in_specs=[vm] * 2 + [hbm] * 7,
            out_specs=vm,
            scratch_shapes=[
                pltpu.VMEM((B, F), BF16),
                pltpu.VMEM((B, F), BF16),
                pltpu.VMEM((F, B), BF16),
                pltpu.VMEM((B, F), BF16),
                pltpu.VMEM((B, F), BF16),
                pltpu.VMEM((F, B), BF16),
                pltpu.VMEM((T, D), BF16),
                pltpu.VMEM((Z, TP, B), BF16),
                pltpu.VMEM((8, NS), F32),
                pltpu.VMEM((Z, TP, B), BF16),
                pltpu.VMEM((H, 8, NS), F32),
                pltpu.VMEM((H, NS, B), BF16),
                pltpu.VMEM((Z, NS, B), BF16),
                pltpu.VMEM((2, 2, NS, FH), F32),
                pltpu.VMEM((2, H, 2, 2, NS, FH), jnp.int16),
                pltpu.VMEM((2, H, 2, 2, NS, FH), jnp.int16),
                pltpu.VMEM((2, H, 2, 2 * T, FH), jnp.int16),
                pltpu.VMEM((2, H, 2, 2 * T, FH), jnp.int16),
                pltpu.VMEM((Z, 2, NS, FH), BF16),
                pltpu.VMEM((Z, 2, TP, FH), BF16),
                pltpu.VMEM((H, NS, B), F32),
                pltpu.VMEM((H, NS, B), BF16),
                pltpu.VMEM((H, NS, B), BF16),
                pltpu.VMEM((H, TP, B), F32),
                pltpu.VMEM((H, TP, B), F32),
                pltpu.VMEM((H, TP, B), F32),
                pltpu.VMEM((H, NS, B), BF16),
                pltpu.VMEM((H, NS, B), BF16),
                pltpu.VMEM((H, TP, B), BF16),
                pltpu.VMEM((Z, TP, B), BF16),
                dma((6,)), dma(()),
                dma((H,)), dma((H,)), dma((H,)), dma((H,)), dma((H,)), dma((H,)), dma((H,)), dma((H,)), dma((H,)), dma((H,)),
                dma((2, H, 2, 2)), dma((2, H, 2, 2)), dma((2, H, 2)), dma((2, H, 2)),
                dma((2, 2, H)), dma((2, 2, H)), dma((2, 2, H)), dma((2, 2, H)),
                dma((H,)), dma((H,)), dma((H,)), dma((H,)), dma((H,)), dma((H,)), dma((H, 2)), dma((2, H)),
            ],
            compiler_params=pltpu.CompilerParams(
                collective_id=0, has_side_effects=True, vmem_limit_bytes=60 * 1024 * 1024
            ),
            name="moe_layer",
        )(ids.T, rw.T, tokens, wg.reshape(wg.shape[1:]), wu.reshape(wu.shape[1:]), wd.reshape(wd.shape[1:]), sg, su, sd)

    placed = (
        P(("dp", "expert"), None),
        P(("dp", "expert"), None),
        P(("dp", "expert"), None),
        P("expert", "dp", "tensor"),
        P("expert", "dp", "tensor"),
        P("expert", "tensor", "dp"),
        P("dp", "tensor"),
        P("dp", "tensor"),
        P("tensor", "dp"),
    )
    return jax.shard_map(
        per_device, mesh=mesh, in_specs=placed, out_specs=P(("dp", "expert"), None), check_vma=False
    )
```

```python
import functools

import jax
import jax.numpy as jnp
from jax import lax
from jax.experimental import pallas as pl
from jax.experimental.pallas import tpu as pltpu
from jax.sharding import PartitionSpec as P

CAP = 8
TP = 16
MESH = pl.DeviceIdType.MESH
F32 = jnp.float32
BF16 = jnp.bfloat16


def dot(a, b):
    return jnp.dot(a, b, preferred_element_type=F32)


CODES = 237.0
LOWEST = 126.0
LOG2E = 1.4426950408889634


def code(v):
    c = jnp.maximum((jnp.log(jnp.abs(v)) * LOG2E + LOWEST) * CODES + 0.5, 0.0).astype(jnp.int32)
    return jnp.where(v < 0.0, -c, c).astype(jnp.int16)


def value(coded):
    c = coded.astype(jnp.int32)
    v = jnp.exp2(jnp.abs(c).astype(F32) * (1.0 / CODES) - LOWEST)
    return jnp.where(c > 0, v, jnp.where(c < 0, -v, 0.0))


def layer_kernel(
    Z, E, T, B, FH,
    ids_ref, rw_ref, tok_hbm, wg_hbm, wu_hbm, wd_hbm, sg_hbm, su_hbm, sd_hbm,
    out_ref,
    wg, wu, wd, sg, su, sd,
    tok, tb, tw, xs, xw, pk, x, p, sb, rb, ssb, srb, hid, hs, acc, os_, orc, sac, sos, sor, oo, rr, fb, ob,
    l_sem, t_sem, a_ss, a_rs, v_ss, v_rs, w_ss, w_rs, b_ss, b_rs, f_ss, f_rs,
    c_ss, c_rs, d_ss, d_rs, g_ss, g_rs, h_ss, h_rs, o_ss, o_rs, q_ss, q_rs, r_ss, r_rs, y_ss, y_rs,
):
    H = Z // 2
    NS = E * CAP
    z, e, t = lax.axis_index("dp"), lax.axis_index("expert"), lax.axis_index("tensor")
    zr, zl = lax.rem(z + 1, Z), lax.rem(z + Z - 1, Z)
    far = lax.rem(z + H, Z)
    pt = 1 - t

    barrier = pltpu.get_barrier_semaphore()
    for j in range(1, Z):
        zz = lax.rem(z + j, Z)
        for tt in range(2):
            pl.semaphore_signal(barrier, inc=1, device_id=(zz, e, tt), device_id_type=MESH)
    for j in range(1, E):
        ee = lax.rem(e + j, E)
        pl.semaphore_signal(barrier, inc=1, device_id=(z, ee, t), device_id_type=MESH)
    pl.semaphore_signal(barrier, inc=1, device_id=(z, e, pt), device_id_type=MESH)

    def chunk(i, core):
        return lax.rem(z + (1 - core) * (Z - i) + core * (1 + i), Z)

    def at(way, k):
        return lax.rem(z + Z - k, Z) if way == 0 else lax.rem(z + k, Z)

    def owner_home(way, j):
        return lax.rem(z + Z - j + H, Z) if way == 0 else lax.rem(z + j + H, Z)

    def remote(src, dst, ss, rs, dev):
        return pltpu.make_async_remote_copy(
            src_ref=src, dst_ref=dst, send_sem=ss, recv_sem=rs, device_id=dev, device_id_type=MESH
        )

    def next_to(way):
        return (zr if way == 0 else zl, e, t)

    def take(ref, sem):
        pltpu.make_async_copy(ref, ref, sem).wait()

    def rows(j):
        return pl.ds(pl.multiple_of(j * CAP, CAP), CAP)

    tok_load = pltpu.make_async_copy(tok_hbm, tok, t_sem)
    tok_load.start()
    loads = [
        pltpu.make_async_copy(src, dst, l_sem.at[n])
        for n, (src, dst) in enumerate(
            ((sg_hbm, sg), (su_hbm, su), (wg_hbm, wg), (wu_hbm, wu), (wd_hbm, wd), (sd_hbm, sd))
        )
    ]

    ids = ids_ref[...]
    rw = rw_ref[...]
    slot = lax.broadcasted_iota(jnp.int32, (NS, T), 0)
    named = lax.shift_right_logical(slot, 3)
    m = jnp.zeros((NS, T), F32)
    weight = jnp.zeros((NS, T), F32)
    for k in range(ids.shape[0]):
        hit = ids[k : k + 1, :] == named
        m = m + jnp.where(hit, 1.0, 0.0)
        weight = weight + jnp.where(hit, rw[k : k + 1, :], 0.0)
    token = lax.broadcasted_iota(jnp.int32, (NS, T), 1)
    before = jnp.zeros((NS, T), F32)
    for r in range(T - 1):
        before = before + jnp.where(token > r, m[:, r : r + 1], 0.0)
    placed = jnp.where(before == (slot & 7).astype(F32), m, 0.0)
    which = jnp.sum(placed * (token + 1).astype(F32), axis=1, keepdims=True) - 1.0
    weight = jnp.sum(placed * weight, axis=1, keepdims=True)
    tw[...] = jnp.concatenate([which, weight, jnp.zeros((NS, NS - 2), F32)], axis=1).T[0:8, :]
    for d in range(Z):
        tb[d, 8:TP, :] = jnp.zeros((TP - 8, B), BF16)
    tok_load.wait()
    for load in loads:
        load.start()
    for d in range(Z):
        tb[d, 0:T, :] = tok[:, d * B : (d + 1) * B]

    pl.semaphore_wait(barrier, 2 * (Z - 1) + (E - 1) + 1)

    def copies_a(i):
        d = lax.rem(z + (1 - t) * i + t * (Z - 1 - i), Z)
        return (
            remote(tw, xw.at[i], w_ss.at[i], w_rs.at[i], (d, e, t)),
            remote(tb.at[d], xs.at[z], a_ss.at[i], a_rs.at[i], (d, e, t)),
        )

    def start_a(i):
        for c in copies_a(i):
            c.start()

    def copy_v(i):
        c = chunk(i, t)
        return remote(xs.at[c], xs.at[c], v_ss.at[i], v_rs.at[i], (z, e, pt))

    def named_by(i):
        return lax.broadcasted_iota(jnp.int32, (TP, NS), 0).astype(F32) == xw[i, 0:1, :]

    def pick(i):
        zc = chunk(i, t)
        cb = jnp.where(named_by(i), 1.0, 0.0).astype(BF16)
        picked = lax.dot_general(cb, xs[zc], (((0,), (0,)), ((), ())), preferred_element_type=F32)
        pk[i] = picked.astype(BF16)

        def send_b(k, carry):
            ee = lax.rem(e + k, E)
            remote(pk.at[i, rows(ee)], x.at[zc, rows(e)], b_ss.at[i], b_rs.at[i], (z, ee, t)).start()
            return carry

        lax.fori_loop(1, E, send_b, 0)
        x[zc, rows(e), :] = pk[i, rows(e), :]

    def arrive(i):
        take(xw.at[i], w_rs.at[i])
        take(xs.at[0], a_rs.at[i])
        copy_v(i).start()
        pick(i)

    def copy_d(way, k, half):
        return remote(
            ssb.at[way, k, half], srb.at[way, k, half], d_ss.at[way, k, half], d_rs.at[way, k, half], next_to(way)
        )

    def cols(half):
        return slice(half * FH, (half + 1) * FH)

    def pack(g, u):
        return jnp.concatenate([g[0:8], u[0:8], g[8:T], u[8:T]], axis=0)

    def step_s(k, first):
        if first > 0:
            take(xs.at[0], v_rs.at[k - pt])
        for half in range(2):
            ways = (half,) if first == 0 else (0, 1)
            v = [xs[at(way, k)] for way in ways]
            v = v[0] if first == 0 else jnp.concatenate(v, axis=0)
            sums = [dot(v, w[:, cols(half)]) for w in (sg, su)]
            for n, way in enumerate(ways):
                add = first > 1 or (first == 1 and half == way)
                if add:
                    copy_d(way, k - 1, half).wait_recv()
                packed = pack(*[u[n * TP : (n + 1) * TP] for u in sums])
                if add:
                    packed = packed + value(srb[way, k - 1, half])
                ssb[way, k, half] = code(packed)
                copy_d(way, k, half).start()

    def silu_up(g, u):
        return (g / (1.0 + jnp.exp(-g)) * u).astype(BF16)

    def last_s():
        @pl.when(t == 0)
        def _():
            take(xs.at[0], v_rs.at[H - 1])

        for half in range(2):
            for way in range(2):
                copy_d(way, H - 1, half).wait_recv()
            m = pack(dot(xs[far], sg[:, cols(half)]), dot(xs[far], su[:, cols(half)]))
            m = m + value(srb[0, H - 1, half]) + value(srb[1, H - 1, half])
            rest = jnp.zeros((TP - T, FH), F32)
            g = jnp.concatenate([m[0:8], m[16 : 8 + T], rest], axis=0)
            u = jnp.concatenate([m[8:16], m[8 + T : 2 * T], rest], axis=0)
            hs[far, half] = silu_up(g, u)

    xs[z] = tb[z]

    @pl.when(t == 0)
    def _():
        xw[0] = tw[...]
        pick(0)

    @pl.when(t == 1)
    def _():
        start_a(0)

    for i in range(1, H):
        start_a(i)
    for load in loads[:2]:
        load.wait()
    step_s(0, 0)
    arrive(1 - t)
    step_s(1, 1)
    for load in loads[2:4]:
        load.wait()

    def copy_c(way, k, half, q):
        return remote(
            sb.at[way, k, half, q],
            rb.at[way, k, half, q],
            c_ss.at[way, k, half, q],
            c_rs.at[way, k, half, q],
            next_to(way),
        )

    def forward(n):
        zc = chunk(n, t)
        return remote(x.at[zc], x.at[zc], f_ss.at[n], f_rs.at[n], (z, e, pt))

    def pass_on(n):
        take(x.at[chunk(n, t), pl.ds(0, (E - 1) * CAP)], b_rs.at[n])
        forward(n).start()

    def from_partner(n):
        take(x.at[chunk(n, pt)], f_rs.at[n])

    def partial(c, half, q, to):
        p[to, q] = dot(x[c], (wg, wu)[q][:, cols(half)])

    @pl.when(t == 0)
    def _():
        pass_on(0)

    @pl.when(t == 1)
    def _():
        from_partner(0)

    for q in range(2):
        for way in range(2):
            partial(z, way, q, way)
            sb[way, 0, way, q] = code(p[way, q])
            copy_c(way, 0, way, q).start()
    for k in range(2, H):
        arrive(k - t)

    @pl.when(t == 1)
    def _():
        arrive(H - 1)

    def step_c(k, carry):
        pass_on(k - t)
        from_partner(k - pt)
        for half in range(2):
            for q in range(2):
                for way in range(2):
                    partial(at(way, k), half, q, way)

                    def plus(half=half, q=q, way=way):
                        copy_c(way, k - 1, half, q).wait_recv()
                        p[way, q] = p[way, q] + value(rb[way, k - 1, half, q])

                    if half == way:
                        plus()
                    else:
                        pl.when(k > 1)(plus)
                    sb[way, k, half, q] = code(p[way, q])
                    copy_c(way, k, half, q).start()

        @pl.when(k < H - 1)
        def _():
            step_s(k + 1, 2)

        return carry

    lax.fori_loop(1, H, step_c, 0)

    @pl.when(t == 1)
    def _():
        pass_on(H - 1)

    @pl.when(t == 0)
    def _():
        from_partner(H - 1)

    def copy_g(way, half, j):
        c = owner_home(way, j)
        return remote(
            hid.at[c, half], hid.at[c, half], g_ss.at[way, half, j], g_rs.at[way, half, j], next_to(way)
        )

    def copy_h(way, half, j):
        c = owner_home(way, j)
        return remote(hs.at[c, half], hs.at[c, half], h_ss.at[way, half, j], h_rs.at[way, half, j], next_to(way))

    def hop(copy, way, half, j):
        copy(way, half, j - 1).wait_recv()
        if j < H - 1 or (j == H - 1 and half == way):
            copy(way, half, j).start()

    for half in range(2):
        for q in range(2):
            partial(far, half, q, half)
    last_s()
    for half in range(2):
        for way in range(2):
            copy_h(way, half, 0).start()
    for half in range(2):
        for q in range(2):
            for way in range(2):
                copy_c(way, H - 1, half, q).wait_recv()
            p[half, q] = p[half, q] + value(rb[0, H - 1, half, q]) + value(rb[1, H - 1, half, q])
        hid[far, half] = silu_up(p[half, 0], p[half, 1])
        for way in range(2):
            copy_g(way, half, 0).start()

    for load in loads[4:]:
        load.wait()

    def down(v, w):
        return dot(v[0], w[0:FH, :]) + dot(v[1], w[FH : 2 * FH, :])

    def copy_o(i):
        return remote(os_.at[i], orc.at[i], o_ss.at[i], o_rs.at[i], (z, e, pt))

    def copy_q(i):
        return remote(sos.at[i], sor.at[i], q_ss.at[i], q_rs.at[i], (z, e, pt))

    def keep_or_give(i, keeper, c):
        @pl.when(t == keeper)
        def _():
            acc[i] = down(hid[c], wd)

        @pl.when(t != keeper)
        def _():
            os_[i] = down(hid[c], wd).astype(BF16)
            copy_o(i).start()

    def shared_one(i, keeper, c):
        v = down(hs[c], sd)

        @pl.when(t == keeper)
        def _():
            sac[i] = v

        @pl.when(t != keeper)
        def _():
            sos[i] = v
            copy_q(i).start()

    def shared_pair(theirs, mine):
        v = jnp.concatenate([hs[chunk(theirs, pt)], hs[chunk(mine, t)]], axis=1)
        v = down(v, sd)
        sos[theirs] = v[0:TP]
        copy_q(theirs).start()
        sac[mine] = v[TP : 2 * TP]

    def finish(i):
        copy_o(i).wait_recv()
        oo[i] = (acc[i] + orc[i].astype(F32)).astype(BF16)

        def send_r(k, carry):
            ee = lax.rem(e + k, E)
            remote(oo.at[i, rows(ee)], rr.at[i, rows(e)], r_ss.at[i], r_rs.at[i], (z, ee, t)).start()
            return carry

        lax.fori_loop(1, E, send_r, 0)
        rr[i, rows(e), :] = oo[i, rows(e), :]

    def copy_y(i, tt):
        return remote(fb.at[i], ob.at[z], y_ss.at[i, tt], y_rs.at[t, i], (chunk(i, t), e, tt))

    def combine(i):
        take(sor.at[i], q_rs.at[i])
        shared = sac[i] + sor[i]
        take(rr.at[i, pl.ds(0, (E - 1) * CAP)], r_rs.at[i])
        v = lax.dot_general(
            jnp.where(named_by(i), xw[i, 1:2, :], 0.0),
            rr[i].astype(F32),
            (((1,), (0,)), ((), ())),
            precision=lax.Precision.HIGHEST,
            preferred_element_type=F32,
        )
        fb[i] = (v + shared).astype(BF16)

    def go_home(i):
        combine(i)
        copy_y(i, 1).start()
        if i > 0:
            copy_y(i, 0).start()
        else:

            @pl.when(t == 1)
            def _():
                copy_y(0, 0).start()

            @pl.when(t == 0)
            def _():
                ob[z] = fb[0]

    keep_or_give(H - 1, 1, far)
    shared_one(H - 1, 1, far)
    for j in range(1, H):
        mine = H - j - t
        theirs = H - j - pt
        for way in range(2):
            hop(copy_g, way, 0, j)
        if j > 1:
            finish(mine + 1)
        for way in range(2):
            hop(copy_g, way, 1, j)
        os_[theirs] = down(hid[chunk(theirs, pt)], wd).astype(BF16)
        copy_o(theirs).start()
        acc[mine] = down(hid[chunk(mine, t)], wd)
        for half in range(2):
            for way in range(2):
                hop(copy_h, way, half, j)
        if j == 1:

            @pl.when(t == 1)
            def _():
                finish(H - 1)

        shared_pair(theirs, mine)
    finish(1 - t)
    if H > 2:
        go_home(H - 1)
    copy_g(0, 0, H - 1).wait_recv()
    copy_g(1, 1, H - 1).wait_recv()
    keep_or_give(0, 0, z)
    @pl.when(t == 0)
    def _():
        finish(0)

    copy_h(0, 0, H - 1).wait_recv()
    copy_h(1, 1, H - 1).wait_recv()
    shared_one(0, 0, z)

    for i in range(H - 1 if H == 2 else H - 2, -1, -1):
        go_home(i)

    for src in range(2):
        for i in range(H):
            if src == 0 and i == 0:

                @pl.when(t == 1)
                def _():
                    take(ob.at[0], y_rs.at[0, 0])

            else:
                take(ob.at[0], y_rs.at[src, i])
    for d in range(Z):
        out_ref[:, d * B : (d + 1) * B] = ob[d, 0:T, :]

    def sent_a(i):
        for c in copies_a(i):
            c.wait_send()
        copy_v(i).wait_send()

    for i in range(H):
        take(pk.at[i, pl.ds(0, (E - 1) * CAP)], b_ss.at[i])
        take(oo.at[i, pl.ds(0, (E - 1) * CAP)], r_ss.at[i])
        forward(i).wait_send()
        copy_o(i).wait_send()
        copy_q(i).wait_send()
        copy_y(i, 1).wait_send()
        if i > 0:
            copy_y(i, 0).wait_send()
            sent_a(i)

    @pl.when(t == 1)
    def _():
        copy_y(0, 0).wait_send()
        sent_a(0)

    for k in range(H):
        for half in range(2):
            for way in range(2):
                if k > 0 or half == way:
                    copy_d(way, k, half).wait_send()
                    for q in range(2):
                        copy_c(way, k, half, q).wait_send()
                if k < H - 1 or half == way:
                    copy_g(way, half, k).wait_send()
                    copy_h(way, half, k).wait_send()


def solution(mesh):
    Z, E = mesh.shape["dp"], mesh.shape["expert"]
    H, NS = Z // 2, E * CAP

    def per_device(tokens, ids, rw, wg, wu, wd, sg, su, sd):
        T, D = tokens.shape
        B, F = sg.shape
        FH = F // 2
        dma = pltpu.SemaphoreType.DMA
        vm = pl.BlockSpec(memory_space=pltpu.VMEM)
        hbm = pl.BlockSpec(memory_space=pl.ANY)
        return pl.pallas_call(
            functools.partial(layer_kernel, Z, E, T, B, FH),
            out_shape=jax.ShapeDtypeStruct((T, D), BF16),
            in_specs=[vm] * 2 + [hbm] * 7,
            out_specs=vm,
            scratch_shapes=[
                pltpu.VMEM((B, F), BF16),
                pltpu.VMEM((B, F), BF16),
                pltpu.VMEM((F, B), BF16),
                pltpu.VMEM((B, F), BF16),
                pltpu.VMEM((B, F), BF16),
                pltpu.VMEM((F, B), BF16),
                pltpu.VMEM((T, D), BF16),
                pltpu.VMEM((Z, TP, B), BF16),
                pltpu.VMEM((8, NS), F32),
                pltpu.VMEM((Z, TP, B), BF16),
                pltpu.VMEM((H, 8, NS), F32),
                pltpu.VMEM((H, NS, B), BF16),
                pltpu.VMEM((Z, NS, B), BF16),
                pltpu.VMEM((2, 2, NS, FH), F32),
                pltpu.VMEM((2, H, 2, 2, NS, FH), jnp.int16),
                pltpu.VMEM((2, H, 2, 2, NS, FH), jnp.int16),
                pltpu.VMEM((2, H, 2, 2 * T, FH), jnp.int16),
                pltpu.VMEM((2, H, 2, 2 * T, FH), jnp.int16),
                pltpu.VMEM((Z, 2, NS, FH), BF16),
                pltpu.VMEM((Z, 2, TP, FH), BF16),
                pltpu.VMEM((H, NS, B), F32),
                pltpu.VMEM((H, NS, B), BF16),
                pltpu.VMEM((H, NS, B), BF16),
                pltpu.VMEM((H, TP, B), F32),
                pltpu.VMEM((H, TP, B), F32),
                pltpu.VMEM((H, TP, B), F32),
                pltpu.VMEM((H, NS, B), BF16),
                pltpu.VMEM((H, NS, B), BF16),
                pltpu.VMEM((H, TP, B), BF16),
                pltpu.VMEM((Z, TP, B), BF16),
                dma((6,)), dma(()),
                dma((H,)), dma((H,)), dma((H,)), dma((H,)), dma((H,)), dma((H,)), dma((H,)), dma((H,)), dma((H,)), dma((H,)),
                dma((2, H, 2, 2)), dma((2, H, 2, 2)), dma((2, H, 2)), dma((2, H, 2)),
                dma((2, 2, H)), dma((2, 2, H)), dma((2, 2, H)), dma((2, 2, H)),
                dma((H,)), dma((H,)), dma((H,)), dma((H,)), dma((H,)), dma((H,)), dma((H, 2)), dma((2, H)),
            ],
            compiler_params=pltpu.CompilerParams(
                collective_id=0, has_side_effects=True, vmem_limit_bytes=60 * 1024 * 1024
            ),
            name="moe_layer",
        )(ids.T, rw.T, tokens, wg.reshape(wg.shape[1:]), wu.reshape(wu.shape[1:]), wd.reshape(wd.shape[1:]), sg, su, sd)

    placed = (
        P(("dp", "expert"), None),
        P(("dp", "expert"), None),
        P(("dp", "expert"), None),
        P("expert", "dp", "tensor"),
        P("expert", "dp", "tensor"),
        P("expert", "tensor", "dp"),
        P("dp", "tensor"),
        P("dp", "tensor"),
        P("tensor", "dp"),
    )
    return jax.shard_map(
        per_device, mesh=mesh, in_specs=placed, out_specs=P(("dp", "expert"), None), check_vma=False
    )
```
